1024 devices in a mesh: seq: 32 (over y, z_hi, core), et: 32 (over z_lo, x).
Axes of the slice: x: 4, y: 4, z: 32 (z_hi: 4, z_lo: 8; z = z_hi * 8 + z_lo), core: 2. Of those that a mesh axis runs over, the one named last changes fastest.
Arguments:
- hidden_in: bfloat16 [1024, 4096], P('seq'), may hold values from -6 to 6
- expert_ids: int32 [1024, 2], P('seq'), may hold values from 0 to 7, all different within a row; in each aligned block of 32 rows (0 to 31, 32 to 63, ...) at most 10 rows name the same one
- gate_vals: bfloat16 [1024, 2], P('seq'), may hold values from 0 to 1, as said below
- w_gate: bfloat16 [32, 4096, 3584], P('et', None, 'seq'), may hold values from -0.09375 to 0.09375
- w_up: bfloat16 [32, 4096, 3584], P('et', None, 'seq'), may hold values from -0.09375 to 0.09375
- w_down: bfloat16 [32, 3584, 4096], P('et', 'seq'), may hold values from -0.09375 to 0.09375
Outputs:
- mixed: bfloat16 [1024, 4096], P('seq', 'et')
The draws below stay inside these ranges and needn't reach their ends.
Inputs may be any that keep to these rules, and one draw needn't show every extreme that they name: `expert_ids`: the rows of each token name different experts; within each block of 32 rows (the rows of one device) no expert is named by more than 10 rows. `gate_vals`: each token's two weights sum to 1 up to bfloat16 rounding, the first is not the smaller.
All inputs are finite; a program needn't handle non-finite values.
Results may differ from the reference program's by a relative error of at most 0.019.
Values may be sent and summed in bfloat16 or wider, within the bound.
A program may use at most 32 MiB of HBM per device.

```python
import math
import jax
import jax.numpy as jnp
import numpy as np
from jax import lax

D = 4096
FF = 14336
EXPERTS = 8
TOP = 2
TOK_DEV = 32
SLOTS = 10
GROUP = 4
TOKENS = 1024
N_SEQ = 32


def draw_gate_vals(key, part):
    leading = jax.random.uniform(key, (TOKENS, 1), jnp.float32, 0.5, 0.9)
    return jnp.concatenate([leading, 1.0 - leading], axis=1).astype(jnp.bfloat16)


def spiked(drawn, stream_key, source, target, shards_of, factor):
    owner, partner = [(jnp.arange(drawn.shape[dim]) // (drawn.shape[dim] // shards_of)).reshape([-1 if axis == dim else 1 for axis in range(drawn.ndim)]) for dim in (source, target)]
    chosen = jax.random.permutation(stream_key, shards_of)[partner]
    strong = (owner == chosen) | (owner == (partner + shards_of // 2) % shards_of)
    return jnp.where(strong, factor * drawn, drawn)


def block_scale(key, extent, cuts, low, largest):
    gain = 1.0
    for position, shards_of in cuts:
        steps = jax.random.uniform(jax.random.fold_in(jax.random.fold_in(key, 6), position), (shards_of,), jnp.float32, low / len(cuts), largest / len(cuts))
        gain = gain * jnp.repeat(jnp.exp(steps), extent[position] // shards_of).reshape((-1,) + (1,) * (len(extent) - 1 - position))
    return gain


def shared_out(key, own, number, rows, number_of, top, most, slope):
    sequence = jax.random.permutation(key, number_of)
    crowded, usual = shares(number_of, rows * top, most, slope, True), shares(number_of, rows * top, most, slope, False)
    places = jnp.arange(number_of)

    def named(lengths, turn):
        used = int((lengths > 0).sum())
        fixed = max(1, used // 4)
        moved = fixed + (places - fixed + turn * (used - fixed)) % max(1, number_of - fixed)
        return jnp.zeros((number_of,), jnp.int32).at[sequence[jnp.where(places < fixed, places, moved)]].set(jnp.asarray(lengths, jnp.int32))

    lengths = jnp.where(number % 4 == 0, named(crowded, number // 4), named(usual, number - number // 4 - 1))
    mixed = jax.random.permutation(jax.random.fold_in(own, 3), number_of)
    source_of, receiver = mixed[0:number_of // 2 * 2:2], mixed[1:number_of // 2 * 2:2]
    margin = jnp.minimum(lengths[source_of] - 1, most - lengths[receiver]) // 2
    margin = jnp.where((source_of == sequence[0]) | (receiver == sequence[0]) | (lengths[receiver] == 0), 0, jnp.maximum(margin, 0))
    moved = jax.random.randint(jax.random.fold_in(own, 4), (number_of // 2,), 0, 1 << 20) % (margin + 1)
    lengths = lengths.at[source_of].add(-moved).at[receiver].add(moved)
    labels = jnp.searchsorted(jnp.cumsum(lengths), jnp.arange(rows * top), side="right").astype(jnp.int32)
    grid = labels.reshape(top, rows).T
    grid = grid[jax.random.permutation(jax.random.fold_in(own, 1), rows)]
    turn = jax.random.randint(jax.random.fold_in(own, 2), (rows, 1), 0, top)
    return jnp.take_along_axis(grid, (jnp.arange(top)[None, :] + turn) % top, axis=1)


def shares(count, total, reach, slope, full):
    weights = [(1 << 20) // math.isqrt(rank ** slope) + 1 for rank in range(1, count + 1)]
    largest = reach if full else min(reach, max(-(-total // count), total * weights[0] // sum(weights)))
    least = 1 if total - largest >= count - 1 else 0
    holding, rest = [largest] + [least] * (count - 1), total - largest - least * (count - 1)
    while rest > 0:
        free = [i for i in range(1, count) if holding[i] < largest] or [i for i in range(1, count) if holding[i] < reach]
        pool, remaining = sum([weights[i] for i in free]), rest
        for i in free:
            addition = min(reach - holding[i], max(1, remaining * weights[i] // pool), rest)
            holding[i] = holding[i] + addition
            rest = rest - addition
    return np.array(holding)


def scatter_about(own_key, shape, spread, bound, split=(), held_as=jnp.bfloat16):
    array = jax.random.normal(own_key, shape, jnp.float32) * spread
    if len(split) > 0:
        array = block_scale(own_key, shape, split, -0.22, 0.18) * array
    return jnp.clip(array, min=-bound, max=bound).astype(held_as)


def gaussian_with(key, dims, scale, reach, split, heavy, kind=jnp.bfloat16):
    array = scale * jax.random.normal(key, dims, jnp.float32)
    if split:
        array = array * block_scale(key, dims, split, -0.22, 0.18)
    return jnp.clip(spiked(array, jax.random.fold_in(key, 3), *heavy), -reach, reach).astype(kind)


def setup_inputs(seed: int = 0) -> dict:
    key_list = jax.random.split(jax.random.key(seed), 7)
    hidden_in = scatter_about(key_list[0], (TOKENS, D), 1.0, 6.0, ((0, 32),))
    expert_ids_keys = jax.random.split(jax.random.fold_in(key_list[1], 1), TOKENS // TOK_DEV)
    expert_ids_turns = jax.random.permutation(jax.random.fold_in(key_list[1], 3), TOKENS // TOK_DEV)
    expert_ids = jax.vmap(lambda own, number: shared_out(jax.random.fold_in(key_list[1], 2), own, number, TOK_DEV, EXPERTS, TOP, SLOTS, 2))(expert_ids_keys, expert_ids_turns).reshape((TOKENS, TOP))
    gate_vals = draw_gate_vals(jax.random.fold_in(key_list[6], 71), 0)
    w_gate = scatter_about(key_list[3], (EXPERTS * GROUP, D, FF // GROUP), D ** -0.5, 0.09375, ((0, 32), (2, 32)))
    w_up = scatter_about(key_list[4], (EXPERTS * GROUP, D, FF // GROUP), D ** -0.5, 0.09375, ((0, 32), (2, 32)))
    w_down = gaussian_with(key_list[5], (EXPERTS * GROUP, FF // GROUP, D), FF ** -0.5, 0.09375, ((0, 32), (1, 32)), (1, 2, 32, 2.75))
    return {"hidden_in": hidden_in, "expert_ids": expert_ids, "gate_vals": gate_vals, "w_gate": w_gate, "w_up": w_up, "w_down": w_down}


def slot_numbers(routed):
    flattened = routed.reshape(-1)
    one_hot = (flattened[:, None] == jnp.arange(EXPERTS, dtype=jnp.int32)[None, :]).astype(jnp.int32)
    earlier = jnp.cumsum(one_hot, axis=0) - one_hot
    return jnp.sum(earlier * one_hot, axis=1).reshape(routed.shape).astype(jnp.int32)


def reference(hidden_in, expert_ids, gate_vals, w_gate, w_up, w_down):
    group_size = w_gate.shape[0] // EXPERTS
    block_count = hidden_in.shape[0] // TOK_DEV
    run_width = FF // (group_size * N_SEQ)
    stream = hidden_in.reshape(block_count, TOK_DEV, D)
    routed = expert_ids.reshape(block_count, TOK_DEV, TOP)
    gates = gate_vals.astype(jnp.float32).reshape(block_count, TOK_DEV, TOP)
    slot_index = jax.vmap(slot_numbers)(routed)
    expert_range = jnp.arange(EXPERTS, dtype=jnp.int32)
    columns = jnp.arange(SLOTS, dtype=jnp.int32)
    matches = (routed[:, None, None, :, :] == expert_range[None, :, None, None, None]) & (slot_index[:, None, None, :, :] == columns[None, None, :, None, None])
    placing = jnp.sum(matches.astype(jnp.float32), axis=-1)
    combining = jnp.sum(jnp.where(matches, gates[:, None, None, :, :], 0.0), axis=-1)
    buffer = jnp.einsum("bect,btd->becd", placing, stream.astype(jnp.float32)).astype(jnp.bfloat16)
    row_count = block_count * SLOTS

    def run_expert(index):
        selected = buffer[:, index].reshape(row_count, D)
        gate_block = lax.dynamic_slice_in_dim(w_gate, index * group_size, group_size, 0)
        up_block = lax.dynamic_slice_in_dim(w_up, index * group_size, group_size, 0)
        down_block = lax.dynamic_slice_in_dim(w_down, index * group_size, group_size, 0)
        gate_full = jnp.transpose(gate_block, (1, 0, 2)).reshape(D, -1)
        up_full = jnp.transpose(up_block, (1, 0, 2)).reshape(D, -1)
        gate_part = jnp.dot(selected, gate_full, preferred_element_type=jnp.float32)
        up_part = jnp.dot(selected, up_full, preferred_element_type=jnp.float32)
        activations = (jax.nn.silu(gate_part) * up_part).astype(jnp.bfloat16)
        act_runs = jnp.transpose(activations.reshape(row_count, group_size, N_SEQ, run_width), (2, 0, 1, 3))
        down_runs = jnp.transpose(down_block.reshape(group_size, N_SEQ, run_width, D), (1, 0, 2, 3))

        def add_run(total, pair):
            act_run, down_run = pair
            piece = jnp.einsum("rgc,gcd->rgd", act_run.astype(jnp.float32), down_run.astype(jnp.float32), precision=lax.Precision.HIGHEST)
            rounded = lax.optimization_barrier(piece.astype(jnp.bfloat16))
            return total + rounded.astype(jnp.float32), None

        start = jnp.zeros((row_count, group_size, D), jnp.float32)
        total, unused = lax.scan(add_run, start, (act_runs, down_runs))
        return total

    expert_out = lax.map(run_expert, expert_range)
    expert_out = expert_out.reshape(EXPERTS, block_count, SLOTS, group_size, D)
    summed = jnp.einsum("bect,ebcgd->btd", combining, expert_out, precision=lax.Precision.HIGHEST)
    mixed = stream.astype(jnp.float32) + summed
    return mixed.reshape(block_count * TOK_DEV, D).astype(jnp.bfloat16)
```

```python
import functools

import jax
import jax.numpy as jnp
from jax import lax
from jax.experimental import pallas as pl
from jax.experimental.pallas import tpu as pltpu
from jax.sharding import Mesh
from jax.sharding import PartitionSpec as P

EXPERTS = 8
SLOTS = 10
PAIRS = SLOTS // 2
LANES = 128
AXES = ("y", "zh", "c", "zl", "x")
NY, NZH, NC, NZL, NX = 4, 4, 2, 8, 4
SEQ = ("y", "zh", "c")
ET = ("zl", "x")
ROWS = NY * NC * SLOTS
MESH = pl.DeviceIdType.MESH


def moe_kernel(
    hidden_any, ids_ref, gate_ref, wg_any, wu_any, wd_any,
    out_ref,
    hid, wgu, wd, picked, gathered, xbuf, ysend, yrecv, yown, rrecv, total, homeward, arrived, returned,
    load_sem, disp_send, disp_recv, ag_send, ag_recv, fwd_send, fwd_recv,
    pair_send, pair_recv, rs_send, rs_recv, ret_send, ret_recv,
):
    at = {name: lax.axis_index(name) for name in AXES}
    y, zh, c, zl, x = (at[name] for name in AXES)

    def device(**other):
        return {**at, **other}

    def remote(src, dst, send, recv, dev):
        return pltpu.make_async_remote_copy(
            src_ref=src, dst_ref=dst, send_sem=send, recv_sem=recv, device_id=dev, device_id_type=MESH
        )

    def up(v, d, n):
        return lax.rem(v + d, n)

    barrier = pltpu.get_barrier_semaphore()

    def hello(**other):
        pl.semaphore_signal(barrier, inc=1, device_id=device(**other), device_id_type=MESH)

    def hello_plane(p, carry):
        hello(x=up(x, lax.rem(p, NX), NX), y=up(y, p // NX, NY))
        return carry

    def hello_far(p, carry):
        hello(y=up(y, lax.rem(p, NY), NY), c=up(c, p // NY, NC), zh=up(zh, 1, NZH))
        hello(y=up(y, lax.rem(p, NY), NY), c=up(c, p // NY, NC), zh=up(zh, 3, NZH))
        return carry

    def hello_region(p, carry):
        hello(zl=up(zl, p, NZL))
        return carry

    def hello_twin(p, carry):
        hello(y=up(y, p, NY), c=1 - c)
        return carry

    lax.fori_loop(0, NY * NC, hello_far, 0)
    lax.fori_loop(1, NZL, hello_region, 0)
    lax.fori_loop(1, NX * NY, hello_plane, 0)
    lax.fori_loop(0, NY, hello_twin, 0)

    loads = [
        pltpu.make_async_copy(hidden_any, hid, load_sem.at[0]),
        pltpu.make_async_copy(wg_any, wgu.at[pl.ds(0, 112)], load_sem.at[1]),
        pltpu.make_async_copy(wu_any, wgu.at[pl.ds(128, 112)], load_sem.at[2]),
        pltpu.make_async_copy(wd_any, wd.at[pl.ds(0, 112)], load_sem.at[3]),
    ]
    for load in loads:
        load.start()
    width = wd.shape[1]
    wgu[pl.ds(112, 16), :] = jnp.zeros((16, width), jnp.bfloat16)
    wgu[pl.ds(240, 16), :] = jnp.zeros((16, width), jnp.bfloat16)
    wd[pl.ds(112, 16), :] = jnp.zeros((16, width), jnp.bfloat16)

    tokens = ids_ref.shape[1]
    ids = ids_ref[...]
    expert = lax.broadcasted_iota(jnp.int32, (EXPERTS, tokens), 0)
    first, second = ids[0:1, :], ids[1:2, :]
    named = (jnp.where(first == expert, 1.0, 0.0) + jnp.where(second == expert, 1.0, 0.0)).astype(jnp.float32)
    before = jnp.where(
        lax.broadcasted_iota(jnp.int32, (tokens, tokens), 0) < lax.broadcasted_iota(jnp.int32, (tokens, tokens), 1),
        1.0, 0.0,
    ).astype(jnp.float32)
    earlier = jnp.dot(named, before, preferred_element_type=jnp.float32)

    def number(chosen):
        slot = jnp.sum(jnp.where(chosen == expert, earlier, 0.0), axis=0, keepdims=True)
        return chosen * SLOTS + slot.astype(jnp.int32)

    n_first, n_second = number(first), number(second)
    wanted = lax.broadcasted_iota(jnp.int32, (16, tokens), 0)
    wanted = jnp.where(wanted < SLOTS, wanted + zl * SLOTS, -1)
    placing = (
        jnp.where(n_first == wanted, 1.0, 0.0) + jnp.where(n_second == wanted, 1.0, 0.0)
    ).astype(jnp.bfloat16)
    loads[0].wait()
    for j in range(NZL):
        block = hid[:, pl.ds(pl.multiple_of((j * NX + x) * LANES, LANES), LANES)]
        rows = jnp.dot(placing, block, preferred_element_type=jnp.float32)
        for p in range(PAIRS):
            picked[j, p] = rows[2 * p : 2 * p + 2].astype(jnp.bfloat16)

    me = y * NC + c
    pl.semaphore_wait(barrier, 2 * NY * NC + (NZL - 1) + (NX * NY - 1) + NY)

    def to_region(step, group):
        def send(p, carry):
            ty, tc = up(y, lax.rem(p, NY), NY), up(c, p // NY, NC)
            remote(
                picked.at[ty * NC + tc], gathered.at[group, me], disp_send, disp_recv.at[group],
                device(y=ty, c=tc, zh=up(zh, step, NZH)),
            ).start()
            return carry
        return send

    lax.fori_loop(0, NY * NC, to_region(3, 1), 0)
    lax.fori_loop(0, NY * NC, to_region(1, 2), 0)
    lax.fori_loop(1, NY * NC, to_region(0, 0), 0)
    gathered[0, me] = picked[me]

    def mine(group):
        return xbuf.at[group, :, pl.ds(pl.multiple_of((me * NX + x) * LANES, LANES), LANES)]

    def spread(group):
        dst = mine(group)
        for s in range(NY * NC):
            for p in range(PAIRS):
                dst[pl.ds((s * PAIRS + p) * 2, 2), :] = gathered[group, s, p]

        def send(p, carry):
            remote(
                mine(group), mine(group), ag_send, ag_recv.at[group],
                device(x=up(x, lax.rem(p, NX), NX), y=up(y, p // NX, NY)),
            ).start()
            return carry

        lax.fori_loop(1, NX * NY, send, 0)

    def waits(ref, sem):
        pltpu.make_async_copy(ref, ref, sem).wait()

    def run(group, half, ty):
        return xbuf.at[group, :, pl.ds(pl.multiple_of((ty * NC + half) * NX * LANES, LANES), NX * LANES)]

    def forward(group):
        waits(xbuf.at[group, :, pl.ds(0, 15 * LANES)], ag_recv.at[group])
        for ty in range(NY):
            remote(run(group, c, ty), run(group, c, ty), fwd_send, fwd_recv.at[group], device(c=1 - c)).start()

    def compute(group):
        waits(xbuf.at[group, :, pl.ds(0, 16 * LANES)], fwd_recv.at[group])
        h = lax.dot_general(
            xbuf[group], wgu[...], (((1,), (1,)), ((), ())), preferred_element_type=jnp.float32
        )
        g, u = h[:, :128], h[:, 128:]
        act = (g / (1.0 + jnp.exp(-g)) * u).astype(jnp.bfloat16)

        def down(half, ty):
            cols = pl.ds(pl.multiple_of((ty * NC + half) * NX * LANES, LANES), NX * LANES)
            return jnp.dot(act, wd[:, cols], preferred_element_type=jnp.float32)

        for ty in range(NY):
            ysend[group, ty] = down(1 - c, ty).astype(jnp.bfloat16)
            remote(ysend.at[group, ty], yrecv.at[group, ty], pair_send, pair_recv.at[group], device(c=1 - c)).start()
        for ty in range(NY):
            yown[group, ty] = down(c, ty).astype(jnp.bfloat16)

    def scatter(group):
        waits(yrecv.at[group], pair_recv.at[group])
        for ty in range(NY):
            both = yown[group, ty].astype(jnp.float32) + yrecv[group, ty].astype(jnp.float32)
            yown[group, ty] = both.astype(jnp.bfloat16)

        def send(p, carry):
            tx, ty = up(x, lax.rem(p, NX), NX), up(y, p // NX, NY)
            remote(
                yown.at[group, ty, :, pl.ds(pl.multiple_of(tx * LANES, LANES), LANES)],
                rrecv.at[group, p - 1], rs_send, rs_recv.at[group], device(x=tx, y=ty),
            ).start()
            return carry

        lax.fori_loop(1, NX * NY, send, 0)

    def send_home(group, step):
        waits(rrecv.at[group], rs_recv.at[group])
        acc = yown[group, y, :, pl.ds(pl.multiple_of(x * LANES, LANES), LANES)].astype(jnp.float32)
        for s in range(NX * NY - 1):
            acc = acc + rrecv[group, s].astype(jnp.float32)
        total[...] = acc
        for s in range(NY * NC):
            for p in range(PAIRS):
                homeward[group, s, p] = total[pl.ds((s * PAIRS + p) * 2, 2), :].astype(jnp.bfloat16)
        target_zh = up(zh, step, NZH)

        def send(s, carry):
            ty, tc = s // NC, lax.rem(s, NC)
            dst = arrived.at[zh, zl]
            here = (target_zh == zh) & (ty == y) & (tc == c) & (zl == me)

            @pl.when(here)
            def _():
                pltpu.make_async_copy(homeward.at[group, s], dst, ret_recv).start()

            @pl.when(jnp.logical_not(here))
            def _():
                remote(
                    homeward.at[group, s], dst, ret_send, ret_recv,
                    device(y=ty, c=tc, zh=target_zh, zl=me),
                ).start()
            return carry

        lax.fori_loop(0, NY * NC, send, 0)

    waits(gathered.at[0, pl.ds(0, 7)], disp_recv.at[0])
    spread(0)
    forward(0)
    waits(gathered.at[1], disp_recv.at[1])
    remote(
        gathered.at[1, pl.ds(0, 4)], gathered.at[3, pl.ds(0, 4)], disp_send, disp_recv.at[3],
        device(zh=up(zh, 3, NZH)),
    ).start()
    waits(gathered.at[2], disp_recv.at[2])
    remote(
        gathered.at[2, pl.ds(4, 4)], gathered.at[3, pl.ds(4, 4)], disp_send, disp_recv.at[3],
        device(zh=up(zh, 1, NZH)),
    ).start()
    spread(1)
    spread(2)
    for load in loads[1:]:
        load.wait()
    compute(0)
    forward(1)
    scatter(0)
    waits(gathered.at[3], disp_recv.at[3])
    spread(3)
    forward(2)
    compute(1)
    compute(2)
    forward(3)
    scatter(1)
    scatter(2)
    compute(3)
    send_home(0, 0)
    scatter(3)
    send_home(1, 1)
    send_home(2, 3)
    send_home(3, 2)

    waits(arrived, ret_recv)
    for e in range(EXPERTS):
        for p in range(PAIRS):
            part = arrived[0, e, p].astype(jnp.float32)
            for k in range(1, NZH):
                part = part + arrived[k, e, p].astype(jnp.float32)
            returned[pl.ds((e * PAIRS + p) * 2, 2), :] = part
    place = lax.broadcasted_iota(jnp.int32, (EXPERTS * SLOTS, tokens), 0)
    gates = gate_ref[...].astype(jnp.float32)
    combining = jnp.where(n_first == place, gates[0:1, :], 0.0) + jnp.where(n_second == place, gates[1:2, :], 0.0)
    mixed = lax.dot_general(
        combining, returned[...], (((0,), (0,)), ((), ())),
        preferred_element_type=jnp.float32, precision=lax.Precision.HIGHEST,
    )
    residual = hid[:, pl.ds(pl.multiple_of((zl * NX + x) * LANES, LANES), LANES)].astype(jnp.float32)
    out_ref[...] = (residual + mixed).astype(jnp.bfloat16)

    for _ in range(3):
        waits(gathered.at[1], disp_send)
    waits(gathered.at[0, pl.ds(0, 7)], disp_send)
    for group in range(4):
        waits(xbuf.at[group, :, pl.ds(0, 15 * LANES)], ag_send)
        waits(xbuf.at[group, :, pl.ds(0, 16 * LANES)], fwd_send)
        waits(yrecv.at[group], pair_send)
        waits(rrecv.at[group], rs_send)
    waits(arrived.at[pl.ds(0, 3)], ret_send)
    waits(arrived.at[3, pl.ds(0, 7)], ret_send)

    @pl.when(zl != me)
    def _():
        waits(arrived.at[3, 7], ret_send)


def local(hidden_in, expert_ids, gate_vals, w_gate, w_up, w_down):
    tokens, width = hidden_in.shape
    ids = jnp.swapaxes(expert_ids, 0, 1)
    gates = jnp.swapaxes(gate_vals, 0, 1)
    wg = jnp.swapaxes(w_gate[0], 0, 1)
    wu = jnp.swapaxes(w_up[0], 0, 1)
    bf16, f32 = jnp.bfloat16, jnp.float32
    dma, anywhere, vmem = pltpu.SemaphoreType.DMA, pl.BlockSpec(memory_space=pl.ANY), pl.BlockSpec(memory_space=pltpu.VMEM)
    return pl.pallas_call(
        moe_kernel,
        name="moe",
        out_shape=jax.ShapeDtypeStruct((tokens, LANES), bf16),
        in_specs=[anywhere, vmem, vmem, anywhere, anywhere, anywhere],
        out_specs=vmem,
        scratch_shapes=[
            pltpu.VMEM((tokens, width), bf16),
            pltpu.VMEM((256, width), bf16),
            pltpu.VMEM((128, width), bf16),
            pltpu.VMEM((8, PAIRS, 2, LANES), bf16),
            pltpu.VMEM((4, 8, PAIRS, 2, LANES), bf16),
            pltpu.VMEM((4, ROWS, width), bf16),
            pltpu.VMEM((4, NY, ROWS, NX * LANES), bf16),
            pltpu.VMEM((4, NY, ROWS, NX * LANES), bf16),
            pltpu.VMEM((4, NY, ROWS, NX * LANES), bf16),
            pltpu.VMEM((4, NX * NY - 1, ROWS, LANES), bf16),
            pltpu.VMEM((ROWS, LANES), f32),
            pltpu.VMEM((4, 8, PAIRS, 2, LANES), bf16),
            pltpu.VMEM((4, 8, PAIRS, 2, LANES), bf16),
            pltpu.VMEM((ROWS, LANES), f32),
            dma((4,)), dma, dma((4,)), dma, dma((4,)), dma, dma((4,)),
            dma, dma((4,)), dma, dma((4,)), dma, dma,
        ],
        compiler_params=pltpu.CompilerParams(
            collective_id=0, has_side_effects=True, vmem_limit_bytes=40 * 1024 * 1024
        ),
    )(hidden_in, ids, gates, wg, wu, w_down[0])


def solution(mesh):
    split = Mesh(mesh.devices.reshape(NY, NZH, NC, NZL, NX), AXES)
    return jax.shard_map(
        local,
        mesh=split,
        in_specs=(
            P(SEQ, None),
            P(SEQ, None),
            P(SEQ, None),
            P(ET, None, SEQ),
            P(ET, None, SEQ),
            P(ET, SEQ, None),
        ),
        out_specs=P(SEQ, ET),
        check_vma=False,
    )
```

```python
import functools

import jax
import jax.numpy as jnp
from jax import lax
from jax.experimental import pallas as pl
from jax.experimental.pallas import tpu as pltpu
from jax.sharding import Mesh
from jax.sharding import PartitionSpec as P

EXPERTS = 8
SLOTS = 10
PAIRS = SLOTS // 2
LANES = 128
AXES = ("y", "zh", "c", "zl", "x")
NY, NZH, NC, NZL, NX = 4, 4, 2, 8, 4
SEQ = ("y", "zh", "c")
ET = ("zl", "x")
ROWS = NY * NC * SLOTS
MESH = pl.DeviceIdType.MESH


def moe_kernel(
    hidden_any, ids_any, gate_any, wg_any, wu_any, wd_any,
    out_ref,
    hid, ids_ref, gate_ref, wgu, wd, picked, gathered, xbuf, ysend, yrecv, yown, rrecv, total, homeward, arrived, returned,
    load_sem, disp_send, disp_recv, ag_send, ag_recv, fwd_send, fwd_recv,
    pair_send, pair_recv, rs_send, rs_recv, ret_send, ret_recv,
):
    scope = jax.named_scope
    at = {name: lax.axis_index(name) for name in AXES}
    y, zh, c, zl, x = (at[name] for name in AXES)

    def device(**other):
        return {**at, **other}

    def remote(src, dst, send, recv, dev):
        return pltpu.make_async_remote_copy(
            src_ref=src, dst_ref=dst, send_sem=send, recv_sem=recv, device_id=dev, device_id_type=MESH
        )

    def waits(ref, sem):
        pltpu.make_async_copy(ref, ref, sem).wait()

    def up(v, d, n):
        return lax.rem(v + d, n)

    barrier = pltpu.get_barrier_semaphore()

    def hello(**other):
        pl.semaphore_signal(barrier, inc=1, device_id=device(**other), device_id_type=MESH)

    def hello_plane(p, carry):
        hello(x=up(x, lax.rem(p, NX), NX), y=up(y, p // NX, NY))
        return carry

    def hello_far(p, carry):
        hello(y=up(y, lax.rem(p, NY), NY), c=up(c, p // NY, NC), zh=up(zh, 1, NZH))
        hello(y=up(y, lax.rem(p, NY), NY), c=up(c, p // NY, NC), zh=up(zh, 3, NZH))
        return carry

    def hello_region(p, carry):
        hello(zl=up(zl, p, NZL))
        return carry

    def hello_twin(p, carry):
        hello(y=up(y, p, NY), c=1 - c)
        return carry

    lax.fori_loop(0, NY * NC, hello_far, 0)
    lax.fori_loop(1, NZL, hello_region, 0)
    lax.fori_loop(1, NX * NY, hello_plane, 0)
    lax.fori_loop(0, NY, hello_twin, 0)

    loads = [
        pltpu.make_async_copy(ids_any, ids_ref, load_sem.at[4]),
        pltpu.make_async_copy(gate_any, gate_ref, load_sem.at[5]),
        pltpu.make_async_copy(hidden_any, hid, load_sem.at[0]),
        pltpu.make_async_copy(wg_any, wgu.at[pl.ds(0, 112)], load_sem.at[1]),
        pltpu.make_async_copy(wu_any, wgu.at[pl.ds(128, 112)], load_sem.at[2]),
        pltpu.make_async_copy(wd_any, wd.at[pl.ds(0, 112)], load_sem.at[3]),
    ]
    for load in loads:
        load.start()
    width = wd.shape[1]
    wgu[pl.ds(112, 16), :] = jnp.zeros((16, width), jnp.bfloat16)
    wgu[pl.ds(240, 16), :] = jnp.zeros((16, width), jnp.bfloat16)
    wd[pl.ds(112, 16), :] = jnp.zeros((16, width), jnp.bfloat16)
    loads[0].wait()
    loads[1].wait()

    tokens = ids_ref.shape[1]
    ids = ids_ref[...]
    expert = lax.broadcasted_iota(jnp.int32, (EXPERTS, tokens), 0)
    first, second = ids[0:1, :], ids[1:2, :]
    named = (jnp.where(first == expert, 1.0, 0.0) + jnp.where(second == expert, 1.0, 0.0)).astype(jnp.float32)
    before = jnp.where(
        lax.broadcasted_iota(jnp.int32, (tokens, tokens), 0) < lax.broadcasted_iota(jnp.int32, (tokens, tokens), 1),
        1.0, 0.0,
    ).astype(jnp.float32)
    earlier = jnp.dot(named, before, preferred_element_type=jnp.float32)

    def number(chosen):
        slot = jnp.sum(jnp.where(chosen == expert, earlier, 0.0), axis=0, keepdims=True)
        return chosen * SLOTS + slot.astype(jnp.int32)

    n_first, n_second = number(first), number(second)
    wanted = lax.broadcasted_iota(jnp.int32, (16, tokens), 0)
    wanted = jnp.where(wanted < SLOTS, wanted + zl * SLOTS, -1)
    placing = (
        jnp.where(n_first == wanted, 1.0, 0.0) + jnp.where(n_second == wanted, 1.0, 0.0)
    ).astype(jnp.bfloat16)
    loads[2].wait()
    for j in range(NZL):
        block = hid[:, pl.ds(pl.multiple_of((j * NX + x) * LANES, LANES), LANES)]
        rows = jnp.dot(placing, block, preferred_element_type=jnp.float32)
        for p in range(PAIRS):
            picked[j, p] = rows[2 * p : 2 * p + 2].astype(jnp.bfloat16)

    me = y * NC + c
    with scope("w_barrier"):
        pl.semaphore_wait(barrier, 2 * NY * NC + (NZL - 1) + (NX * NY - 1) + NY)

    order = (
        zh,
        jnp.where(zh == 0, 1, 0),
        jnp.where(zh == 0, 3, jnp.where(zh == 1, 2, 1)),
        jnp.where((zh == 1) | (zh == 2), 3, 2),
    )
    ahead, behind, across = up(zh, 1, NZH), up(zh, 3, NZH), up(zh, 2, NZH)

    def to_region(target):
        def send(p, carry):
            ty, tc = up(y, lax.rem(p, NY), NY), up(c, p // NY, NC)
            remote(
                picked.at[ty * NC + tc], gathered.at[zh, me], disp_send, disp_recv.at[zh],
                device(y=ty, c=tc, zh=target),
            ).start()
            return carry
        return send

    lax.fori_loop(0, NY * NC, to_region(ahead), 0)
    lax.fori_loop(0, NY * NC, to_region(behind), 0)
    lax.fori_loop(1, NY * NC, to_region(zh), 0)
    pltpu.make_async_copy(picked.at[me], gathered.at[zh, me], disp_recv.at[zh]).start()

    def block(r, bx, by):
        return xbuf.at[r, :, pl.ds(pl.multiple_of(((by * NC + c) * NX + bx) * LANES, LANES), LANES)]

    def spread(r):
        mine = block(r, x, y)
        for s in range(NY * NC):
            for p in range(PAIRS):
                mine[pl.ds((s * PAIRS + p) * 2, 2), :] = gathered[r, s, p]

        def send(p, carry):
            remote(
                mine, mine, ag_send, ag_recv.at[r, p - 1],
                device(x=up(x, lax.rem(p, NX), NX), y=up(y, p // NX, NY)),
            ).start()
            return carry

        lax.fori_loop(1, NX * NY, send, 0)
        remote(mine, mine, fwd_send, fwd_recv.at[r], device(c=1 - c)).start()

    def collect(r):
        def take(p, carry):
            theirs = block(r, up(x, NX - lax.rem(p, NX), NX), up(y, NY - p // NX, NY))
            waits(theirs, ag_recv.at[r, p - 1])
            remote(theirs, theirs, fwd_send, fwd_recv.at[r], device(c=1 - c)).start()
            return carry

        lax.fori_loop(1, NX * NY, take, 0)

    def run(half, ty):
        return pl.ds(pl.multiple_of((ty * NC + half) * NX * LANES, LANES), NX * LANES)

    def compute(r):
        def up_gate(half):
            parts = [
                lax.dot_general(
                    xbuf[r, :, run(half, ty)], wgu[:, run(half, ty)], (((1,), (1,)), ((), ())),
                    preferred_element_type=jnp.float32,
                )
                for ty in range(NY)
            ]
            return (parts[0] + parts[1]) + (parts[2] + parts[3])

        h = up_gate(c)
        with scope("wfwd"):
            waits(xbuf.at[r, :, pl.ds(0, 16 * LANES)], fwd_recv.at[r])
        h = h + up_gate(1 - c)
        g, u = h[:, :128], h[:, 128:]
        act = (g / (1.0 + jnp.exp(-g)) * u).astype(jnp.bfloat16)
        dys = (2, 1, 3, 0)
        for dy in dys:
            ty = up(y, dy, NY)
            ysend[r, ty] = jnp.dot(act, wd[:, run(1 - c, ty)], preferred_element_type=jnp.float32).astype(jnp.bfloat16)
            remote(ysend.at[r, ty], yrecv.at[r, ty], pair_send, pair_recv.at[r, ty], device(c=1 - c)).start()
        for dy in dys:
            ty = up(y, dy, NY)
            both = jnp.dot(act, wd[:, run(c, ty)], preferred_element_type=jnp.float32)
            with scope("wpair"):
                waits(yrecv.at[r, ty], pair_recv.at[r, ty])
            yown[r, ty] = (both + yrecv[r, ty].astype(jnp.float32)).astype(jnp.bfloat16)
            for dx in (2, 1, 3, 0):
                if dx == 0 and dy == 0:
                    continue
                tx = up(x, dx, NX)
                remote(
                    yown.at[r, ty, :, pl.ds(pl.multiple_of(tx * LANES, LANES), LANES)],
                    rrecv.at[r, dy * NX + dx - 1], rs_send, rs_recv.at[r], device(x=tx, y=ty),
                ).start()

    def send_home(r):
        with scope("wrs"):
            waits(rrecv.at[r], rs_recv.at[r])
        acc = yown[r, y, :, pl.ds(pl.multiple_of(x * LANES, LANES), LANES)].astype(jnp.float32)
        for s in range(NX * NY - 1):
            acc = acc + rrecv[r, s].astype(jnp.float32)
        total[...] = acc
        for s in range(NY * NC):
            for p in range(PAIRS):
                homeward[r, s, p] = total[pl.ds((s * PAIRS + p) * 2, 2), :].astype(jnp.bfloat16)

        def send(s, carry):
            ty, tc = s // NC, lax.rem(s, NC)
            dst = arrived.at[zh, zl]
            here = (r == zh) & (ty == y) & (tc == c) & (zl == me)

            @pl.when(here)
            def _():
                pltpu.make_async_copy(homeward.at[r, s], dst, ret_recv).start()

            @pl.when(jnp.logical_not(here))
            def _():
                remote(
                    homeward.at[r, s], dst, ret_send, ret_recv, device(y=ty, c=tc, zh=r, zl=me),
                ).start()
            return carry

        lax.fori_loop(0, NY * NC, send, 0)

    def far_one(k):
        @pl.when(order[k] == across)
        def _():
            waits(gathered.at[order[k]], disp_recv.at[order[k]])

    with scope("wown"):
        waits(gathered.at[zh], disp_recv.at[zh])
    spread(zh)
    with scope("wnear"):
        waits(gathered.at[ahead], disp_recv.at[ahead])
    remote(
        gathered.at[ahead, pl.ds(0, 4)], gathered.at[ahead, pl.ds(0, 4)], disp_send, disp_recv.at[ahead],
        device(zh=behind),
    ).start()
    with scope("wnear"):
        waits(gathered.at[behind], disp_recv.at[behind])
    remote(
        gathered.at[behind, pl.ds(4, 4)], gathered.at[behind, pl.ds(4, 4)], disp_send, disp_recv.at[behind],
        device(zh=ahead),
    ).start()

    @pl.when(order[1] != across)
    def _():
        spread(order[1])

    with scope("col0"):
        collect(zh)
    for load in loads[3:]:
        load.wait()
    with scope("comp0"):
        compute(zh)

    @pl.when(order[1] == across)
    def _():
        with scope("wfar"):
            waits(gathered.at[order[1]], disp_recv.at[order[1]])
        spread(order[1])

    with scope("col1"):
        collect(order[1])
    far_one(2)
    with scope("spread2"):
        spread(order[2])
    with scope("comp1"):
        compute(order[1])
    with scope("col2"):
        collect(order[2])
    far_one(3)
    with scope("spread3"):
        spread(order[3])
    with scope("home0"):
        send_home(zh)
    with scope("comp2"):
        compute(order[2])
    with scope("home1"):
        send_home(order[1])
    with scope("col3"):
        collect(order[3])
    with scope("comp3"):
        compute(order[3])
    with scope("home2"):
        send_home(order[2])
    with scope("home3"):
        send_home(order[3])

    with scope("wret"):
        waits(arrived, ret_recv)
    for e in range(EXPERTS):
        for p in range(PAIRS):
            part = arrived[0, e, p].astype(jnp.float32)
            for k in range(1, NZH):
                part = part + arrived[k, e, p].astype(jnp.float32)
            returned[pl.ds((e * PAIRS + p) * 2, 2), :] = part
    place = lax.broadcasted_iota(jnp.int32, (EXPERTS * SLOTS, tokens), 0)
    gates = gate_ref[...].astype(jnp.float32)
    combining = jnp.where(n_first == place, gates[0:1, :], 0.0) + jnp.where(n_second == place, gates[1:2, :], 0.0)
    mixed = lax.dot_general(
        combining, returned[...], (((0,), (0,)), ((), ())),
        preferred_element_type=jnp.float32, precision=lax.Precision.HIGHEST,
    )
    residual = hid[:, pl.ds(pl.multiple_of((zl * NX + x) * LANES, LANES), LANES)].astype(jnp.float32)
    out_ref[...] = (residual + mixed).astype(jnp.bfloat16)

    with scope("drain"):
        for _ in range(3):
            waits(gathered.at[1], disp_send)
        waits(gathered.at[0, pl.ds(0, 7)], disp_send)
        for r in range(4):
            waits(xbuf.at[r, :, pl.ds(0, 15 * LANES)], ag_send)
            waits(xbuf.at[r, :, pl.ds(0, 16 * LANES)], fwd_send)
            waits(yrecv.at[r], pair_send)
            waits(rrecv.at[r], rs_send)
        waits(arrived.at[pl.ds(0, 3)], ret_send)
        waits(arrived.at[3, pl.ds(0, 7)], ret_send)

        @pl.when(zl != me)
        def _():
            waits(arrived.at[3, 7], ret_send)


def local(hidden_in, expert_ids, gate_vals, w_gate, w_up, w_down):
    tokens, width = hidden_in.shape
    ids = jnp.swapaxes(expert_ids, 0, 1)
    gates = jnp.swapaxes(gate_vals, 0, 1)
    wg = jnp.swapaxes(w_gate[0], 0, 1)
    wu = jnp.swapaxes(w_up[0], 0, 1)
    bf16, f32 = jnp.bfloat16, jnp.float32
    dma, hbm, vmem = pltpu.SemaphoreType.DMA, pl.BlockSpec(memory_space=pltpu.HBM), pl.BlockSpec(memory_space=pltpu.VMEM)
    return pl.pallas_call(
        moe_kernel,
        name="moe",
        out_shape=jax.ShapeDtypeStruct((tokens, LANES), bf16),
        in_specs=[hbm] * 6,
        out_specs=vmem,
        scratch_shapes=[
            pltpu.VMEM((tokens, width), bf16),
            pltpu.VMEM((2, tokens), jnp.int32),
            pltpu.VMEM((2, tokens), bf16),
            pltpu.VMEM((256, width), bf16),
            pltpu.VMEM((128, width), bf16),
            pltpu.VMEM((8, PAIRS, 2, LANES), bf16),
            pltpu.VMEM((4, 8, PAIRS, 2, LANES), bf16),
            pltpu.VMEM((4, ROWS, width), bf16),
            pltpu.VMEM((4, NY, ROWS, NX * LANES), bf16),
            pltpu.VMEM((4, NY, ROWS, NX * LANES), bf16),
            pltpu.VMEM((4, NY, ROWS, NX * LANES), bf16),
            pltpu.VMEM((4, NX * NY - 1, ROWS, LANES), bf16),
            pltpu.VMEM((ROWS, LANES), f32),
            pltpu.VMEM((4, 8, PAIRS, 2, LANES), bf16),
            pltpu.VMEM((4, 8, PAIRS, 2, LANES), bf16),
            pltpu.VMEM((ROWS, LANES), f32),
            dma((6,)), dma, dma((4,)), dma, dma((4, NX * NY - 1)), dma, dma((4,)),
            dma, dma((4, NY)), dma, dma((4,)), dma, dma,
        ],
        compiler_params=pltpu.CompilerParams(
            collective_id=0, has_side_effects=True, vmem_limit_bytes=67043328
        ),
    )(hidden_in, ids, gates, wg, wu, w_down[0])


def solution(mesh):
    split = Mesh(mesh.devices.reshape(NY, NZH, NC, NZL, NX), AXES)
    return jax.shard_map(
        local,
        mesh=split,
        in_specs=(
            P(SEQ, None),
            P(SEQ, None),
            P(SEQ, None),
            P(ET, None, SEQ),
            P(ET, None, SEQ),
            P(ET, SEQ, None),
        ),
        out_specs=P(SEQ, ET),
        check_vma=False,
    )
```

```python
import functools

import jax
import jax.numpy as jnp
from jax import lax
from jax.experimental import pallas as pl
from jax.experimental.pallas import tpu as pltpu
from jax.sharding import Mesh
from jax.sharding import PartitionSpec as P

EXPERTS = 8
SLOTS = 10
PAIRS = SLOTS // 2
LANES = 128
AXES = ("y", "zh", "c", "zl", "x")
NY, NZH, NC, NZL, NX = 4, 4, 2, 8, 4
SEQ = ("y", "zh", "c")
ET = ("zl", "x")
ROWS = NY * NC * SLOTS
MESH = pl.DeviceIdType.MESH


def moe_kernel(
    hidden_any, ids_any, gate_any, wg_any, wu_any, wd_any,
    out_ref,
    hid, ids_ref, gate_ref, wraw, wup, wdown, picked, gathered, xown, xpair, hidden, ysend, yrecv, yown,
    half, quarter, total, homeward, arrived, returned,
    load_sem, disp_send, disp_recv, ag_send, ag_recv, fwd_send, fwd_recv,
    pair_send, pair_recv, half_send, half_recv, quarter_send, quarter_recv, ret_send, ret_recv,
):
    scope = jax.named_scope
    at = {name: lax.axis_index(name) for name in AXES}
    y, zh, c, zl, x = (at[name] for name in AXES)

    def device(**other):
        return {**at, **other}

    def remote(src, dst, send, recv, dev):
        return pltpu.make_async_remote_copy(
            src_ref=src, dst_ref=dst, send_sem=send, recv_sem=recv, device_id=dev, device_id_type=MESH
        )

    def waits(ref, sem):
        pltpu.make_async_copy(ref, ref, sem).wait()

    def up(v, d, n):
        return lax.rem(v + d, n)

    barrier = pltpu.get_barrier_semaphore()

    def hello(**other):
        pl.semaphore_signal(barrier, inc=1, device_id=device(**other), device_id_type=MESH)

    def hello_plane(p, carry):
        hello(x=up(x, lax.rem(p, NX), NX), y=up(y, p // NX, NY))
        return carry

    def hello_far(p, carry):
        hello(y=up(y, lax.rem(p, NY), NY), c=up(c, p // NY, NC), zh=up(zh, 1, NZH))
        hello(y=up(y, lax.rem(p, NY), NY), c=up(c, p // NY, NC), zh=up(zh, 3, NZH))
        return carry

    def hello_region(p, carry):
        hello(zl=up(zl, p, NZL))
        return carry

    def hello_twin(p, carry):
        hello(y=up(y, p, NY), c=1 - c)
        return carry

    lax.fori_loop(0, NY * NC, hello_far, 0)
    lax.fori_loop(1, NZL, hello_region, 0)
    lax.fori_loop(1, NX * NY, hello_plane, 0)
    lax.fori_loop(0, NY, hello_twin, 0)

    def columns(side, ty):
        core = c if side == 0 else 1 - c
        return pl.ds(pl.multiple_of((ty * NC + core) * NX * LANES, LANES), NX * LANES)

    small = [
        pltpu.make_async_copy(ids_any, ids_ref, load_sem.at[0]),
        pltpu.make_async_copy(gate_any, gate_ref, load_sem.at[1]),
        pltpu.make_async_copy(hidden_any, hid, load_sem.at[2]),
    ]
    loads = []
    for side in range(NC):
        for ty in range(NY):
            to = pl.ds(ty * NX * LANES, NX * LANES)
            loads += [
                pltpu.make_async_copy(wg_any.at[:, columns(side, ty)], wraw.at[side, pl.ds(0, 112), to], load_sem.at[3]),
                pltpu.make_async_copy(wu_any.at[:, columns(side, ty)], wraw.at[side, pl.ds(128, 112), to], load_sem.at[3]),
                pltpu.make_async_copy(wd_any.at[:, columns(side, ty)], wdown.at[side, pl.ds(0, 112), to], load_sem.at[4]),
            ]
    for load in small + loads:
        load.start()
    width = wdown.shape[2]
    for side in range(NC):
        wraw[side, pl.ds(112, 16), :] = jnp.zeros((16, width), jnp.bfloat16)
        wraw[side, pl.ds(240, 16), :] = jnp.zeros((16, width), jnp.bfloat16)
        wdown[side, pl.ds(112, 16), :] = jnp.zeros((16, width), jnp.bfloat16)
    small[0].wait()
    small[1].wait()

    tokens = ids_ref.shape[1]
    ids = ids_ref[...]
    expert = lax.broadcasted_iota(jnp.int32, (EXPERTS, tokens), 0)
    first, second = ids[0:1, :], ids[1:2, :]
    named = (jnp.where(first == expert, 1.0, 0.0) + jnp.where(second == expert, 1.0, 0.0)).astype(jnp.float32)
    before = jnp.where(
        lax.broadcasted_iota(jnp.int32, (tokens, tokens), 0) < lax.broadcasted_iota(jnp.int32, (tokens, tokens), 1),
        1.0, 0.0,
    ).astype(jnp.float32)
    earlier = jnp.dot(named, before, preferred_element_type=jnp.float32)

    def number(chosen):
        slot = jnp.sum(jnp.where(chosen == expert, earlier, 0.0), axis=0, keepdims=True)
        return chosen * SLOTS + slot.astype(jnp.int32)

    n_first, n_second = number(first), number(second)
    wanted = lax.broadcasted_iota(jnp.int32, (16, tokens), 0)
    wanted = jnp.where(wanted < SLOTS, wanted + zl * SLOTS, -1)
    placing = (
        jnp.where(n_first == wanted, 1.0, 0.0) + jnp.where(n_second == wanted, 1.0, 0.0)
    ).astype(jnp.bfloat16)
    small[2].wait()
    for j in range(NZL):
        block = hid[:, pl.ds(pl.multiple_of((j * NX + x) * LANES, LANES), LANES)]
        rows = jnp.dot(placing, block, preferred_element_type=jnp.float32)
        for p in range(PAIRS):
            picked[j, p] = rows[2 * p : 2 * p + 2].astype(jnp.bfloat16)

    me = y * NC + c
    with scope("w_barrier"):
        pl.semaphore_wait(barrier, 2 * NY * NC + (NZL - 1) + (NX * NY - 1) + NY)

    ahead, behind, across = up(zh, 1, NZH), up(zh, 3, NZH), up(zh, 2, NZH)
    odd = lax.rem(zh, 2)
    order = (zh, 1 - odd, 3 - odd, across)

    def to_region(target):
        def send(p, carry):
            ty, tc = up(y, lax.rem(p, NY), NY), up(c, p // NY, NC)
            remote(
                picked.at[ty * NC + tc], gathered.at[zh, me], disp_send, disp_recv.at[zh],
                device(y=ty, c=tc, zh=target),
            ).start()
            return carry
        return send

    lax.fori_loop(0, NY * NC, to_region(ahead), 0)
    lax.fori_loop(0, NY * NC, to_region(behind), 0)
    lax.fori_loop(1, NY * NC, to_region(zh), 0)
    pltpu.make_async_copy(picked.at[me], gathered.at[zh, me], disp_recv.at[zh]).start()

    def shifted(da, db):
        return up(x, da * (1 - c) + db * c, NX), up(y, da * c + db * (1 - c), NY)

    def piece(buf, r, bx, by):
        return buf.at[r, :, pl.ds(pl.multiple_of((by * NX + bx) * LANES, LANES), LANES)]

    def hand_over(r, bx, by):
        remote(piece(xown, r, bx, by), piece(xpair, r, bx, by), fwd_send, fwd_recv.at[r], device(c=1 - c)).start()

    def spread(r):
        mine = piece(xown, r, x, y)
        for s in range(NY * NC):
            for p in range(PAIRS):
                mine[pl.ds((s * PAIRS + p) * 2, 2), :] = gathered[r, s, p]

        def send(d, carry):
            ax, ay = shifted(d, 0)
            remote(mine, mine, ag_send, ag_recv.at[r, d - 1], device(x=ax, y=ay)).start()
            bx, by = shifted(0, d)
            remote(mine, mine, ag_send, ag_recv.at[r, d * NX - 1], device(x=bx, y=by)).start()
            return carry

        lax.fori_loop(1, NX, send, 0)
        hand_over(r, x, y)

    def relay(r):
        def take(da, carry):
            sx, sy = shifted(NX - da, 0)
            theirs = piece(xown, r, sx, sy)
            waits(theirs, ag_recv.at[r, da - 1])

            def send(db, inner):
                bx, by = shifted(0, db)
                remote(theirs, theirs, ag_send, ag_recv.at[r, db * NX + da - 1], device(x=bx, y=by)).start()
                return inner

            lax.fori_loop(1, NY, send, 0)
            hand_over(r, sx, sy)
            return carry

        lax.fori_loop(1, NX, take, 0)

    def collect(r):
        def take(p, carry):
            sx, sy = shifted(lax.rem(NX - lax.rem(p, NX), NX), NY - p // NX)
            waits(piece(xown, r, sx, sy), ag_recv.at[r, p - 1])
            hand_over(r, sx, sy)
            return carry

        lax.fori_loop(NX, NX * NY, take, 0)

    def up_and_down(r):
        h = jnp.dot(xown[r], wup[0], preferred_element_type=jnp.float32)
        with scope("wfwd"):
            waits(xpair.at[r], fwd_recv.at[r])
        h = h + jnp.dot(xpair[r], wup[1], preferred_element_type=jnp.float32)
        g, u = h[:, :128], h[:, 128:]
        act = (g / (1.0 + jnp.exp(-g)) * u).astype(jnp.bfloat16)
        hidden[r] = act
        out = jnp.dot(act, wdown[1], preferred_element_type=jnp.float32).astype(jnp.bfloat16)
        for ty in range(NY):
            for tx in range(NX):
                col = (ty * NX + tx) * LANES
                ysend[r, tx * (1 - c) + ty * c, ty * (1 - c) + tx * c] = out[:, col : col + LANES]
        remote(ysend.at[r], yrecv.at[r], pair_send, pair_recv.at[r], device(c=1 - c)).start()

    mine_b, mine_a = y * (1 - c) + x * c, x * (1 - c) + y * c

    def halve(r):
        out = jnp.dot(hidden[r], wdown[0], preferred_element_type=jnp.float32)
        with scope("wpair"):
            waits(yrecv.at[r], pair_recv.at[r])
        for ty in range(NY):
            for tx in range(NX):
                col = (ty * NX + tx) * LANES
                b, a = ty * (1 - c) + tx * c, tx * (1 - c) + ty * c
                yown[r, b, a] = (out[:, col : col + LANES] + yrecv[r, b, a].astype(jnp.float32)).astype(jnp.bfloat16)

        def send(db, carry):
            bx, by = shifted(0, db)
            remote(
                yown.at[r, up(mine_b, db, NY)], half.at[r, db - 1], half_send, half_recv.at[r], device(x=bx, y=by)
            ).start()
            return carry

        lax.fori_loop(1, NY, send, 0)

    def quarter_sum(r):
        with scope("whalf"):
            waits(half.at[r], half_recv.at[r])
        for a in range(NX):
            acc = yown[r, mine_b, a].astype(jnp.float32)
            for k in range(NY - 1):
                acc = acc + half[r, k, a].astype(jnp.float32)
            yown[r, mine_b, a] = acc.astype(jnp.bfloat16)

        def send(da, carry):
            ax, ay = shifted(da, 0)
            remote(
                yown.at[r, mine_b, up(mine_a, da, NX)], quarter.at[r, da - 1], quarter_send, quarter_recv.at[r],
                device(x=ax, y=ay),
            ).start()
            return carry

        lax.fori_loop(1, NX, send, 0)

    def send_home(r):
        with scope("wquart"):
            waits(quarter.at[r], quarter_recv.at[r])
        acc = yown[r, mine_b, mine_a].astype(jnp.float32)
        for k in range(NX - 1):
            acc = acc + quarter[r, k].astype(jnp.float32)
        total[...] = acc
        for s in range(NY * NC):
            for p in range(PAIRS):
                homeward[r, s, p] = total[pl.ds((s * PAIRS + p) * 2, 2), :].astype(jnp.bfloat16)

        def send(s, carry):
            ty, tc = s // NC, lax.rem(s, NC)
            dst = arrived.at[zh, zl]
            here = (r == zh) & (ty == y) & (tc == c) & (zl == me)

            @pl.when(here)
            def _():
                pltpu.make_async_copy(homeward.at[r, s], dst, ret_recv).start()

            @pl.when(jnp.logical_not(here))
            def _():
                remote(
                    homeward.at[r, s], dst, ret_send, ret_recv, device(y=ty, c=tc, zh=r, zl=me),
                ).start()
            return carry

        lax.fori_loop(0, NY * NC, send, 0)

    own, near_1, near_2, far = order

    with scope("wraw"):
        waits(wraw.at[:, pl.ds(0, 224)], load_sem.at[3])
        waits(wdown.at[:, pl.ds(0, 112)], load_sem.at[4])
    for side in range(NC):
        wup[side] = wraw[side].T
    with scope("wown"):
        waits(gathered.at[own], disp_recv.at[own])
    spread(own)
    with scope("F0"):
        relay(own)
    with scope("wnear"):
        waits(gathered.at[ahead], disp_recv.at[ahead])
    remote(
        gathered.at[ahead, pl.ds(0, 4)], gathered.at[ahead, pl.ds(0, 4)], disp_send, disp_recv.at[ahead],
        device(zh=behind),
    ).start()
    with scope("wnear"):
        waits(gathered.at[behind], disp_recv.at[behind])
    remote(
        gathered.at[behind, pl.ds(4, 4)], gathered.at[behind, pl.ds(4, 4)], disp_send, disp_recv.at[behind],
        device(zh=ahead),
    ).start()
    with scope("S1"):
        spread(near_1)
    with scope("S2"):
        spread(near_2)
    with scope("G0"):
        collect(own)
    with scope("A0"):
        up_and_down(own)
    with scope("F1"):
        relay(near_1)
    with scope("F2"):
        relay(near_2)
    with scope("B0"):
        halve(own)
    with scope("G1"):
        collect(near_1)
    with scope("wfar"):
        waits(gathered.at[far], disp_recv.at[far])
    with scope("S3"):
        spread(far)
    with scope("A1"):
        up_and_down(near_1)
    with scope("Q0"):
        quarter_sum(own)
    with scope("B1"):
        halve(near_1)
    with scope("F3"):
        relay(far)
    with scope("G2"):
        collect(near_2)
    with scope("A2"):
        up_and_down(near_2)
    with scope("Z0"):
        send_home(own)
    with scope("B2"):
        halve(near_2)
    with scope("Q1"):
        quarter_sum(near_1)
    with scope("G3"):
        collect(far)
    with scope("A3"):
        up_and_down(far)
    with scope("Z1"):
        send_home(near_1)
    with scope("Q2"):
        quarter_sum(near_2)
    with scope("B3"):
        halve(far)
    with scope("Z2"):
        send_home(near_2)
    with scope("Q3"):
        quarter_sum(far)
    with scope("Z3"):
        send_home(far)

    with scope("wret"):
        waits(arrived, ret_recv)
    for e in range(EXPERTS):
        for p in range(PAIRS):
            part = arrived[0, e, p].astype(jnp.float32)
            for k in range(1, NZH):
                part = part + arrived[k, e, p].astype(jnp.float32)
            returned[pl.ds((e * PAIRS + p) * 2, 2), :] = part
    place = lax.broadcasted_iota(jnp.int32, (EXPERTS * SLOTS, tokens), 0)
    gates = gate_ref[...].astype(jnp.float32)
    combining = jnp.where(n_first == place, gates[0:1, :], 0.0) + jnp.where(n_second == place, gates[1:2, :], 0.0)
    mixed = lax.dot_general(
        combining, returned[...], (((0,), (0,)), ((), ())),
        preferred_element_type=jnp.float32, precision=lax.Precision.HIGHEST,
    )
    residual = hid[:, pl.ds(pl.multiple_of((zl * NX + x) * LANES, LANES), LANES)].astype(jnp.float32)
    out_ref[...] = (residual + mixed).astype(jnp.bfloat16)

    with scope("drain"):
        for _ in range(3):
            waits(gathered.at[1], disp_send)
        waits(gathered.at[0, pl.ds(0, 7)], disp_send)
        for r in range(4):
            waits(xown.at[r, :, pl.ds(0, 15 * LANES)], ag_send)
            waits(xown.at[r], fwd_send)
            waits(yrecv.at[r], pair_send)
            waits(half.at[r], half_send)
            waits(quarter.at[r], quarter_send)
        waits(arrived.at[pl.ds(0, 3)], ret_send)
        waits(arrived.at[3, pl.ds(0, 7)], ret_send)

        @pl.when(zl != me)
        def _():
            waits(arrived.at[3, 7], ret_send)


def local(hidden_in, expert_ids, gate_vals, w_gate, w_up, w_down):
    tokens, width = hidden_in.shape
    ids = jnp.swapaxes(expert_ids, 0, 1)
    gates = jnp.swapaxes(gate_vals, 0, 1)
    wg = jnp.swapaxes(w_gate[0], 0, 1)
    wu = jnp.swapaxes(w_up[0], 0, 1)
    bf16, f32 = jnp.bfloat16, jnp.float32
    dma, hbm, vmem = pltpu.SemaphoreType.DMA, pl.BlockSpec(memory_space=pltpu.HBM), pl.BlockSpec(memory_space=pltpu.VMEM)
    return pl.pallas_call(
        moe_kernel,
        name="moe",
        out_shape=jax.ShapeDtypeStruct((tokens, LANES), bf16),
        in_specs=[hbm] * 6,
        out_specs=vmem,
        scratch_shapes=[
            pltpu.VMEM((tokens, width), bf16),
            pltpu.VMEM((2, tokens), jnp.int32),
            pltpu.VMEM((2, tokens), bf16),
            pltpu.VMEM((2, 256, width // 2), bf16),
            pltpu.VMEM((2, width // 2, 256), bf16),
            pltpu.VMEM((2, 128, width // 2), bf16),
            pltpu.VMEM((8, PAIRS, 2, LANES), bf16),
            pltpu.VMEM((4, 8, PAIRS, 2, LANES), bf16),
            pltpu.VMEM((4, ROWS, width // 2), bf16),
            pltpu.VMEM((4, ROWS, width // 2), bf16),
            pltpu.VMEM((4, ROWS, LANES), bf16),
            pltpu.VMEM((4, NY, NX, ROWS, LANES), bf16),
            pltpu.VMEM((4, NY, NX, ROWS, LANES), bf16),
            pltpu.VMEM((4, NY, NX, ROWS, LANES), bf16),
            pltpu.VMEM((4, NY - 1, NX, ROWS, LANES), bf16),
            pltpu.VMEM((4, NX - 1, ROWS, LANES), bf16),
            pltpu.VMEM((ROWS, LANES), f32),
            pltpu.VMEM((4, 8, PAIRS, 2, LANES), bf16),
            pltpu.VMEM((4, 8, PAIRS, 2, LANES), bf16),
            pltpu.VMEM((ROWS, LANES), f32),
            dma((5,)), dma, dma((4,)), dma, dma((4, NX * NY - 1)), dma, dma((4,)),
            dma, dma((4,)), dma, dma((4,)), dma, dma((4,)), dma, dma,
        ],
        compiler_params=pltpu.CompilerParams(
            collective_id=0, has_side_effects=True, vmem_limit_bytes=48 * 1024 * 1024
        ),
    )(*(pltpu.with_memory_space_constraint(a, pltpu.HBM) for a in (hidden_in, ids, gates, wg, wu, w_down[0])))


def solution(mesh):
    split = Mesh(mesh.devices.reshape(NY, NZH, NC, NZL, NX), AXES)
    return jax.shard_map(
        local,
        mesh=split,
        in_specs=(
            P(SEQ, None),
            P(SEQ, None),
            P(SEQ, None),
            P(ET, None, SEQ),
            P(ET, None, SEQ),
            P(ET, SEQ, None),
        ),
        out_specs=P(SEQ, ET),
        check_vma=False,
    )
```

```python
import jax
import jax.numpy as jnp
from jax import lax
from jax.experimental import pallas as pl
from jax.experimental.pallas import tpu as pltpu
from jax.sharding import Mesh
from jax.sharding import PartitionSpec as P

EXPERTS = 8
SLOTS = 10
PAIRS = SLOTS // 2
LANES = 128
AXES = ("y", "zh", "c", "zl", "x")
NY, NZH, NC, NZL, NX = 4, 4, 2, 8, 4
SEQ = ("y", "zh", "c")
ET = ("zl", "x")
ROWS = NY * SLOTS
UNITS = 112
PLANE = NX * NY
MESH = pl.DeviceIdType.MESH


def moe_kernel(
    hidden_any, ids_any, gate_any, wg_any, wu_any, wd_any,
    out_ref,
    hid, ids_ref, gate_ref, wraw, wup, wdown, picked, passed, gathered, xbuf, ybuf, summed, total, homeward, arrived, returned,
    load_sem, twin_send, twin_recv, leg_recv, disp_send, disp_recv, ag_send, ag_recv, rs_send, rs_recv, ret_send, ret_recv,
):
    scope = jax.named_scope
    at = {name: lax.axis_index(name) for name in AXES}
    y, zh, c, zl, x = (at[name] for name in AXES)

    def device(**other):
        return {**at, **other}

    def remote(src, dst, send, recv, dev):
        return pltpu.make_async_remote_copy(
            src_ref=src, dst_ref=dst, send_sem=send, recv_sem=recv, device_id=dev, device_id_type=MESH
        )

    def waits(ref, sem):
        pltpu.make_async_copy(ref, ref, sem).wait()

    def up(v, d, n):
        return lax.rem(v + d, n)

    ahead, behind, across = up(zh, 1, NZH), up(zh, 3, NZH), up(zh, 2, NZH)

    barrier = pltpu.get_barrier_semaphore()

    def hello(**other):
        pl.semaphore_signal(barrier, inc=1, device_id=device(**other), device_id_type=MESH)

    def hello_near(d, carry):
        hello(y=up(y, d, NY), zh=ahead)
        hello(y=up(y, d, NY), zh=behind)
        return carry

    high, relays = zl >= NZL // 2, (zl >= 2) & (zl < 6)

    def along(step):
        z = lax.rem(zh * NZL + zl + step + NZH * NZL, NZH * NZL)
        return {"zh": z // NZL, "zl": lax.rem(z, NZL)}

    def hello_relay(d, carry):
        hello(y=up(y, d, NY), **along(jnp.where(high, 6, -6)))
        return carry

    def hello_line(d, carry):
        hello(zl=up(zl, d, NZL))
        return carry

    def hello_plane(p, carry):
        hello(x=up(x, lax.rem(p, NX), NX), y=up(y, p // NX, NY))
        return carry

    lax.fori_loop(0, NY, hello_near, 0)
    lax.fori_loop(0, NY, hello_relay, 0)

    @pl.when(relays)
    def _():
        hello(**along(6))
        hello(**along(-6))

    lax.fori_loop(1, NZL, hello_line, 0)
    lax.fori_loop(1, PLANE, hello_plane, 0)
    hello(c=1 - c)

    width = wdown.shape[2]
    small = [
        pltpu.make_async_copy(ids_any, ids_ref, load_sem.at[0]),
        pltpu.make_async_copy(gate_any, gate_ref, load_sem.at[1]),
        pltpu.make_async_copy(hidden_any, hid, load_sem.at[2]),
    ]
    parts = []
    for h in range(2):
        for ty in range(NY):
            cols, to = pl.ds((2 * ty + h) * NX * LANES, NX * LANES), pl.ds(ty * NX * LANES, NX * LANES)
            for k, (weight, buf, own, twin) in enumerate(
                ((wg_any, wraw, 0, 256), (wu_any, wraw, 128, 384), (wd_any, wdown, 0, 128))
            ):
                parts.append((
                    weight.at[:, cols], buf.at[h, pl.ds(own, UNITS), to], buf.at[h, pl.ds(twin, UNITS), to], 3 + k // 2
                ))
    loads = [pltpu.make_async_copy(part, own, load_sem.at[sem]) for part, own, _, sem in parts]
    for load in small + loads:
        load.start()
    blank = jnp.zeros((128 - UNITS, width), jnp.bfloat16)
    for h in range(2):
        for k in range(4):
            wraw[h, pl.ds(k * 128 + UNITS, 128 - UNITS), :] = blank
        for k in range(2):
            wdown[h, pl.ds(k * 128 + UNITS, 128 - UNITS), :] = blank
    small[0].wait()
    small[1].wait()

    tokens = ids_ref.shape[1]
    ids = ids_ref[...]
    expert = lax.broadcasted_iota(jnp.int32, (EXPERTS, tokens), 0)
    first, second = ids[0:1, :], ids[1:2, :]
    named = (jnp.where(first == expert, 1.0, 0.0) + jnp.where(second == expert, 1.0, 0.0)).astype(jnp.float32)
    before = jnp.where(
        lax.broadcasted_iota(jnp.int32, (tokens, tokens), 0) < lax.broadcasted_iota(jnp.int32, (tokens, tokens), 1),
        1.0, 0.0,
    ).astype(jnp.float32)
    earlier = jnp.dot(named, before, preferred_element_type=jnp.float32)

    def number(chosen):
        slot = jnp.sum(jnp.where(chosen == expert, earlier, 0.0), axis=0, keepdims=True)
        return chosen * SLOTS + slot.astype(jnp.int32)

    n_first, n_second = number(first), number(second)
    slot = lax.broadcasted_iota(jnp.int32, (16, tokens), 0)

    def placing(expert_here):
        wanted = jnp.where(slot < SLOTS, slot + expert_here * SLOTS, -1)
        return (
            jnp.where(n_first == wanted, 1.0, 0.0) + jnp.where(n_second == wanted, 1.0, 0.0)
        ).astype(jnp.bfloat16)

    places = jnp.concatenate([placing(zl), placing(lax.rem(zl + NZL // 2, NZL))], axis=0)
    small[2].wait()
    for j in range(NZL):
        block = hid[:, pl.ds(pl.multiple_of((j * NX + x) * LANES, LANES), LANES)]
        rows = jnp.dot(places, block, preferred_element_type=jnp.float32)
        for k in range(2):
            for p in range(PAIRS):
                picked[k, j // 2, j % 2, p] = rows[16 * k + 2 * p : 16 * k + 2 * p + 2].astype(jnp.bfloat16)

    with scope("w_barrier"):
        pl.semaphore_wait(barrier, 2 * NY + (NZL - 1) + (PLANE - 1) + 2 + jnp.where(relays, 2 * NY, 0))

    order = (
        jnp.where(zh == 0, 0, jnp.where(zh == 1, 1, jnp.where(zh == 2, 2, 3))),
        jnp.where(zh == 0, 1, jnp.where(zh == 1, 0, jnp.where(zh == 2, 1, 0))),
        jnp.where(zh == 0, 3, jnp.where(zh == 1, 2, jnp.where(zh == 2, 0, 2))),
        jnp.where(zh == 0, 2, jnp.where(zh == 1, 3, jnp.where(zh == 2, 3, 1))),
    )
    work = (
        jnp.where(zh == 0, 0, jnp.where(zh == 1, 1, jnp.where(zh == 2, 0, 3))),
        jnp.where(zh == 0, 1, jnp.where(zh == 1, 0, jnp.where(zh == 2, 1, 0))),
        jnp.where(zh == 0, 3, jnp.where(zh == 1, 2, jnp.where(zh == 2, 2, 2))),
        jnp.where(zh == 0, 2, jnp.where(zh == 1, 3, jnp.where(zh == 2, 3, 1))),
    )

    @pl.when(high)
    def _():
        remote(picked.at[1], passed.at[0], disp_send, leg_recv.at[0], device(**along(6))).start()

    @pl.when(jnp.logical_not(high))
    def _():
        remote(picked.at[1], passed.at[1], disp_send, leg_recv.at[1], device(**along(-6))).start()

    def to_region(target):
        def send(d, carry):
            ty = up(y, d, NY)
            remote(
                picked.at[0, ty], gathered.at[zh, y], disp_send, disp_recv.at[zh], device(y=ty, zh=target)
            ).start()
            return carry
        return send

    @pl.when(c == 0)
    def _():
        lax.fori_loop(0, NY, to_region(jnp.where(high, ahead, behind)), 0)

    lax.fori_loop(1, NY, to_region(zh), 0)
    pltpu.make_async_copy(picked.at[0, y], gathered.at[zh, y], disp_recv.at[zh]).start()

    def second_leg(way, source, step):
        waits(passed.at[way], leg_recv.at[way])

        def send(d, carry):
            ty = up(y, d, NY)
            remote(
                passed.at[way, ty], gathered.at[source, y], disp_send, disp_recv.at[source], device(y=ty, **along(step))
            ).start()
            return carry

        lax.fori_loop(0, NY, send, 0)

    def piece(r, tx, ty):
        return xbuf.at[r, :, :, pl.ds(pl.multiple_of((ty * NX + tx) * LANES, LANES), LANES)]

    def spread(r):
        mine = piece(r, x, y)
        for s in range(NY):
            for h in range(2):
                for p in range(PAIRS):
                    mine[h, pl.ds((s * PAIRS + p) * 2, 2), :] = gathered[r, s, h, p]

        def send(p, carry):
            remote(
                mine, mine, ag_send, ag_recv.at[r], device(x=up(x, lax.rem(p, NX), NX), y=up(y, p // NX, NY))
            ).start()
            return carry

        lax.fori_loop(1, PLANE, send, 0)

    def compute(r):
        with scope("wag"):
            waits(xbuf.at[r, :, :, pl.ds(0, (PLANE - 1) * LANES)], ag_recv.at[r])
        up_gate = jnp.dot(xbuf[r, 0], wup[0], preferred_element_type=jnp.float32)
        up_gate = up_gate + jnp.dot(xbuf[r, 1], wup[1], preferred_element_type=jnp.float32)

        def swish(k):
            g, u = up_gate[:, k * 256 : k * 256 + 128], up_gate[:, k * 256 + 128 : k * 256 + 256]
            return (g / (1.0 + jnp.exp(-g)) * u).astype(jnp.bfloat16)

        act = jnp.concatenate([swish(0), swish(1)], axis=1)
        for dy in (2, 1, 3, 0):
            ty = up(y, dy, NY)
            cols = pl.ds(pl.multiple_of(ty * NX * LANES, NX * LANES), NX * LANES)
            for h in range(2):
                out = jnp.dot(act, wdown[h, :, cols], preferred_element_type=jnp.float32).astype(jnp.bfloat16)
                for tx in range(NX):
                    ybuf[r, ty, tx, h] = out[:, tx * LANES : (tx + 1) * LANES]
            for dx in (2, 1, 3, 0):
                if dx == 0 and dy == 0:
                    continue
                tx = up(x, dx, NX)
                remote(
                    ybuf.at[r, ty, tx], summed.at[r, dy * NX + dx - 1], rs_send, rs_recv.at[r], device(x=tx, y=ty)
                ).start()

    def send_home(r):
        with scope("wrs"):
            waits(summed.at[r], rs_recv.at[r])
        acc = ybuf[r, y, x].astype(jnp.float32)
        for s in range(PLANE - 1):
            acc = acc + summed[r, s].astype(jnp.float32)
        total[...] = acc
        for s in range(NY):
            for h in range(2):
                for p in range(PAIRS):
                    homeward[r, s, h, p] = total[h, pl.ds((s * PAIRS + p) * 2, 2), :].astype(jnp.bfloat16)

        def send(k, carry):
            ty, h = k // 2, lax.rem(k, 2)
            tz = 2 * y + h
            dst = arrived.at[zh, zl]
            here = (r == zh) & (ty == y) & (tz == zl)

            @pl.when(here)
            def _():
                pltpu.make_async_copy(homeward.at[r, ty, h], dst, ret_recv).start()

            @pl.when(jnp.logical_not(here))
            def _():
                remote(homeward.at[r, ty, h], dst, ret_send, ret_recv, device(y=ty, zh=r, zl=tz)).start()
            return carry

        lax.fori_loop(0, 2 * NY, send, 0)

    with scope("wraw"):
        waits(wraw.at[:, pl.ds(0, 2 * UNITS)], load_sem.at[3])
        waits(wdown.at[:, pl.ds(0, UNITS)], load_sem.at[4])
    for h in range(2):
        wup[h, :, pl.ds(0, 256)] = wraw[h, pl.ds(0, 256), :].T

    @pl.when(c == 0)
    def _():
        lax.fori_loop(0, NY, to_region(jnp.where(high, behind, ahead)), 0)

    with scope("wS0"):
        waits(gathered.at[order[0]], disp_recv.at[order[0]])
    with scope("S0"):
        spread(order[0])
    @pl.when(c == 1)
    def _():
        lax.fori_loop(0, NY, to_region(ahead), 0)
        lax.fori_loop(0, NY, to_region(behind), 0)

    with scope("R"):
        @pl.when(relays & (zh == 3))
        def _():
            second_leg(1, ahead, -6)

        @pl.when(relays)
        def _():
            second_leg(0, behind, 6)

        @pl.when(relays & (zh != 3))
        def _():
            second_leg(1, ahead, -6)

    for part, _, twin, _ in parts:
        remote(part, twin, twin_send, twin_recv, device(c=1 - c)).start()
    with scope("wS1"):
        waits(gathered.at[order[1]], disp_recv.at[order[1]])
    with scope("S1"):
        spread(order[1])
    with scope("wtwin"):
        waits(wraw.at[:, pl.ds(0, 3 * UNITS)], twin_recv)
    for h in range(2):
        wup[h, :, pl.ds(256, 256)] = wraw[h, pl.ds(256, 256), :].T
    with scope("wS2"):
        waits(gathered.at[order[2]], disp_recv.at[order[2]])
    with scope("S2"):
        spread(order[2])
    @pl.when(zh == 0)
    def _():
        with scope("A0"):
            compute(work[0])
        with scope("wS3"):
            waits(gathered.at[order[3]], disp_recv.at[order[3]])
        with scope("S3"):
            spread(order[3])
        with scope("A1"):
            compute(work[1])
        with scope("A2"):
            compute(work[2])
        with scope("Z0"):
            send_home(work[0])
        with scope("A3"):
            compute(work[3])
        with scope("Z1"):
            send_home(work[1])
        with scope("Z2"):
            send_home(work[2])
        with scope("Z3"):
            send_home(work[3])

    @pl.when(zh != 0)
    def _():
        with scope("A0"):
            compute(work[0])
        with scope("wS3"):
            waits(gathered.at[order[3]], disp_recv.at[order[3]])
        with scope("S3"):
            spread(order[3])
        with scope("A1"):
            compute(work[1])
        with scope("Z0"):
            send_home(work[0])
        with scope("A2"):
            compute(work[2])
        with scope("Z1"):
            send_home(work[1])
        with scope("A3"):
            compute(work[3])
        with scope("Z2"):
            send_home(work[2])
        with scope("Z3"):
            send_home(work[3])

    with scope("wret"):
        waits(arrived, ret_recv)
    for e in range(EXPERTS):
        for p in range(PAIRS):
            part = arrived[0, e, p].astype(jnp.float32)
            for k in range(1, NZH):
                part = part + arrived[k, e, p].astype(jnp.float32)
            returned[pl.ds((e * PAIRS + p) * 2, 2), :] = part
    place = lax.broadcasted_iota(jnp.int32, (EXPERTS * SLOTS, tokens), 0)
    gates = gate_ref[...].astype(jnp.float32)
    combining = jnp.where(n_first == place, gates[0:1, :], 0.0) + jnp.where(n_second == place, gates[1:2, :], 0.0)
    mixed = lax.dot_general(
        combining, returned[...], (((0,), (0,)), ((), ())),
        preferred_element_type=jnp.float32, precision=lax.Precision.HIGHEST,
    )
    residual = hid[:, pl.ds(pl.multiple_of((zl * NX + x) * LANES, LANES), LANES)].astype(jnp.float32)
    out_ref[...] = (residual + mixed).astype(jnp.bfloat16)

    with scope("drain"):
        waits(wraw.at[:, pl.ds(0, 3 * UNITS)], twin_send)
        for _ in range(3):
            waits(gathered.at[1], disp_send)
        waits(gathered.at[0, pl.ds(0, 3)], disp_send)

        @pl.when(relays)
        def _():
            waits(gathered.at[pl.ds(0, 2)], disp_send)

        for r in range(NZH):
            waits(xbuf.at[r, :, :, pl.ds(0, (PLANE - 1) * LANES)], ag_send)
            waits(summed.at[r], rs_send)
        waits(arrived.at[pl.ds(0, 3)], ret_send)
        waits(arrived.at[3, pl.ds(0, 7)], ret_send)

        @pl.when((zl != 2 * y) & (zl != 2 * y + 1))
        def _():
            waits(arrived.at[3, 7], ret_send)


def local(hidden_in, expert_ids, gate_vals, w_gate, w_up, w_down):
    tokens, width = hidden_in.shape
    ids = jnp.swapaxes(expert_ids, 0, 1)
    gates = jnp.swapaxes(gate_vals, 0, 1)
    wg = jnp.swapaxes(w_gate[0], 0, 1)
    wu = jnp.swapaxes(w_up[0], 0, 1)
    bf16, f32 = jnp.bfloat16, jnp.float32
    dma, hbm, vmem = pltpu.SemaphoreType.DMA, pl.BlockSpec(memory_space=pltpu.HBM), pl.BlockSpec(memory_space=pltpu.VMEM)
    return pl.pallas_call(
        moe_kernel,
        name="moe",
        out_shape=jax.ShapeDtypeStruct((tokens, LANES), bf16),
        in_specs=[hbm] * 6,
        out_specs=vmem,
        scratch_shapes=[
            pltpu.VMEM((tokens, width), bf16),
            pltpu.VMEM((2, tokens), jnp.int32),
            pltpu.VMEM((2, tokens), bf16),
            pltpu.VMEM((2, 512, width // 2), bf16),
            pltpu.VMEM((2, width // 2, 512), bf16),
            pltpu.VMEM((2, 256, width // 2), bf16),
            pltpu.VMEM((2, NY, 2, PAIRS, 2, LANES), bf16),
            pltpu.VMEM((2, NY, 2, PAIRS, 2, LANES), bf16),
            pltpu.VMEM((NZH, NY, 2, PAIRS, 2, LANES), bf16),
            pltpu.VMEM((NZH, 2, ROWS, width // 2), bf16),
            pltpu.VMEM((NZH, NY, NX, 2, ROWS, LANES), bf16),
            pltpu.VMEM((NZH, PLANE - 1, 2, ROWS, LANES), bf16),
            pltpu.VMEM((2, ROWS, LANES), f32),
            pltpu.VMEM((NZH, NY, 2, PAIRS, 2, LANES), bf16),
            pltpu.VMEM((NZH, NZL, PAIRS, 2, LANES), bf16),
            pltpu.VMEM((EXPERTS * SLOTS, LANES), f32),
            dma((5,)), dma, dma, dma((2,)), dma, dma((4,)), dma, dma((4,)), dma, dma((4,)), dma, dma,
        ],
        compiler_params=pltpu.CompilerParams(
            collective_id=0, has_side_effects=True, vmem_limit_bytes=48 * 1024 * 1024
        ),
    )(*(pltpu.with_memory_space_constraint(a, pltpu.HBM) for a in (hidden_in, ids, gates, wg, wu, w_down[0])))


def solution(mesh):
    split = Mesh(mesh.devices.reshape(NY, NZH, NC, NZL, NX), AXES)
    return jax.shard_map(
        local,
        mesh=split,
        in_specs=(
            P(SEQ, None),
            P(SEQ, None),
            P(SEQ, None),
            P(ET, None, SEQ),
            P(ET, None, SEQ),
            P(ET, SEQ, None),
        ),
        out_specs=P(SEQ, ET),
        check_vma=False,
    )
```

```python
import jax
import jax.numpy as jnp
from jax import lax
from jax.experimental import pallas as pl
from jax.experimental.pallas import tpu as pltpu
from jax.sharding import Mesh
from jax.sharding import PartitionSpec as P

EXPERTS = 8
SLOTS = 10
PAIRS = SLOTS // 2
LANES = 128
AXES = ("y", "zh", "c", "zl", "x")
NY, NZH, NC, NZL, NX = 4, 4, 2, 8, 4
SEQ = ("y", "zh", "c")
ET = ("zl", "x")
ROWS = NY * SLOTS
UNITS = 112
PLANE = NX * NY
MESH = pl.DeviceIdType.MESH


def moe_kernel(
    hidden_any, ids_any, gate_any, wg_any, wu_any, wd_any,
    out_ref,
    hid, ids_ref, gate_ref, wraw, wup, wdown, picked, passed, gathered, xbuf, ybuf, half, quarter, whole, total, homeward, arrived, returned,
    load_sem, twin_send, twin_recv, leg_recv, disp_send, disp_recv, ag_send, ag_recv,
    half_send, half_recv, quarter_send, quarter_recv, whole_send, whole_recv, ret_send, ret_recv,
):
    scope = jax.named_scope
    at = {name: lax.axis_index(name) for name in AXES}
    y, zh, c, zl, x = (at[name] for name in AXES)

    def device(**other):
        return {**at, **other}

    def remote(src, dst, send, recv, dev):
        return pltpu.make_async_remote_copy(
            src_ref=src, dst_ref=dst, send_sem=send, recv_sem=recv, device_id=dev, device_id_type=MESH
        )

    def waits(ref, sem):
        pltpu.make_async_copy(ref, ref, sem).wait()

    def up(v, d, n):
        return lax.rem(v + d, n)

    ahead, behind, across = up(zh, 1, NZH), up(zh, 3, NZH), up(zh, 2, NZH)

    barrier = pltpu.get_barrier_semaphore()

    def hello(**other):
        pl.semaphore_signal(barrier, inc=1, device_id=device(**other), device_id_type=MESH)

    def hello_near(d, carry):
        hello(y=up(y, d, NY), zh=ahead)
        hello(y=up(y, d, NY), zh=behind)
        return carry

    high, relays = zl >= NZL // 2, (zl >= 2) & (zl < 6)

    def along(step):
        z = lax.rem(zh * NZL + zl + step + NZH * NZL, NZH * NZL)
        return {"zh": z // NZL, "zl": lax.rem(z, NZL)}

    def hello_relay(d, carry):
        hello(y=up(y, d, NY), **along(jnp.where(high, 6, -6)))
        return carry

    def hello_line(d, carry):
        hello(zl=up(zl, d, NZL))
        return carry

    def hello_plane(p, carry):
        hello(x=up(x, lax.rem(p, NX), NX), y=up(y, p // NX, NY))
        return carry

    lax.fori_loop(0, NY, hello_near, 0)
    lax.fori_loop(0, NY, hello_relay, 0)

    @pl.when(relays)
    def _():
        hello(**along(6))
        hello(**along(-6))

    lax.fori_loop(1, NZL, hello_line, 0)
    lax.fori_loop(1, PLANE, hello_plane, 0)
    hello(c=1 - c)

    width = wdown.shape[2]
    small = [
        pltpu.make_async_copy(ids_any, ids_ref, load_sem.at[0]),
        pltpu.make_async_copy(gate_any, gate_ref, load_sem.at[1]),
        pltpu.make_async_copy(hidden_any, hid, load_sem.at[2]),
    ]
    parts = []
    for h in range(2):
        for ty in range(NY):
            cols, to = pl.ds((2 * ty + h) * NX * LANES, NX * LANES), pl.ds(ty * NX * LANES, NX * LANES)
            for k, (weight, buf, own, twin) in enumerate(
                ((wg_any, wraw, 0, 256), (wu_any, wraw, 128, 384), (wd_any, wdown, 0, 128))
            ):
                parts.append((
                    weight.at[:, cols], buf.at[h, pl.ds(own, UNITS), to], buf.at[h, pl.ds(twin, UNITS), to], 3 + k // 2
                ))
    loads = [pltpu.make_async_copy(part, own, load_sem.at[sem]) for part, own, _, sem in parts]
    for load in small + loads:
        load.start()
    blank = jnp.zeros((128 - UNITS, width), jnp.bfloat16)
    for h in range(2):
        for k in range(4):
            wraw[h, pl.ds(k * 128 + UNITS, 128 - UNITS), :] = blank
        for k in range(2):
            wdown[h, pl.ds(k * 128 + UNITS, 128 - UNITS), :] = blank
    small[0].wait()
    small[1].wait()

    tokens = ids_ref.shape[1]
    ids = ids_ref[...]
    expert = lax.broadcasted_iota(jnp.int32, (EXPERTS, tokens), 0)
    first, second = ids[0:1, :], ids[1:2, :]
    named = (jnp.where(first == expert, 1.0, 0.0) + jnp.where(second == expert, 1.0, 0.0)).astype(jnp.float32)
    before = jnp.where(
        lax.broadcasted_iota(jnp.int32, (tokens, tokens), 0) < lax.broadcasted_iota(jnp.int32, (tokens, tokens), 1),
        1.0, 0.0,
    ).astype(jnp.float32)
    earlier = jnp.dot(named, before, preferred_element_type=jnp.float32)

    def number(chosen):
        slot = jnp.sum(jnp.where(chosen == expert, earlier, 0.0), axis=0, keepdims=True)
        return chosen * SLOTS + slot.astype(jnp.int32)

    n_first, n_second = number(first), number(second)
    slot = lax.broadcasted_iota(jnp.int32, (16, tokens), 0)

    def placing(expert_here):
        wanted = jnp.where(slot < SLOTS, slot + expert_here * SLOTS, -1)
        return (
            jnp.where(n_first == wanted, 1.0, 0.0) + jnp.where(n_second == wanted, 1.0, 0.0)
        ).astype(jnp.bfloat16)

    places = jnp.concatenate([placing(zl), placing(lax.rem(zl + NZL // 2, NZL))], axis=0)
    small[2].wait()
    for j in range(NZL):
        block = hid[:, pl.ds(pl.multiple_of((j * NX + x) * LANES, LANES), LANES)]
        rows = jnp.dot(places, block, preferred_element_type=jnp.float32)
        for k in range(2):
            for p in range(PAIRS):
                picked[k, j // 2, j % 2, p] = rows[16 * k + 2 * p : 16 * k + 2 * p + 2].astype(jnp.bfloat16)

    with scope("w_barrier"):
        pl.semaphore_wait(barrier, 2 * NY + (NZL - 1) + (PLANE - 1) + 2 + jnp.where(relays, 2 * NY, 0))

    order = (
        jnp.where(zh == 0, 0, jnp.where(zh == 1, 1, jnp.where(zh == 2, 2, 3))),
        jnp.where(zh == 0, 1, jnp.where(zh == 1, 0, jnp.where(zh == 2, 1, 0))),
        jnp.where(zh == 0, 3, jnp.where(zh == 1, 2, jnp.where(zh == 2, 0, 1))),
        jnp.where(zh == 0, 2, jnp.where(zh == 1, 3, jnp.where(zh == 2, 3, 2))),
    )
    work = (
        jnp.where(zh == 0, 0, jnp.where(zh == 1, 1, jnp.where(zh == 2, 0, 3))),
        jnp.where(zh == 0, 1, jnp.where(zh == 1, 0, jnp.where(zh == 2, 1, 0))),
        jnp.where(zh == 0, 3, jnp.where(zh == 1, 2, jnp.where(zh == 2, 2, 1))),
        jnp.where(zh == 0, 2, jnp.where(zh == 1, 3, jnp.where(zh == 2, 3, 2))),
    )

    @pl.when(high)
    def _():
        remote(picked.at[1], passed.at[0], disp_send, leg_recv.at[0], device(**along(6))).start()

    @pl.when(jnp.logical_not(high))
    def _():
        remote(picked.at[1], passed.at[1], disp_send, leg_recv.at[1], device(**along(-6))).start()

    def to_region(target):
        def send(d, carry):
            ty = up(y, d, NY)
            remote(
                picked.at[0, ty], gathered.at[zh, y], disp_send, disp_recv.at[zh], device(y=ty, zh=target)
            ).start()
            return carry
        return send

    @pl.when(c == 0)
    def _():
        lax.fori_loop(0, NY, to_region(jnp.where(high, ahead, behind)), 0)

    lax.fori_loop(1, NY, to_region(zh), 0)
    pltpu.make_async_copy(picked.at[0, y], gathered.at[zh, y], disp_recv.at[zh]).start()

    def second_leg(way, source, step):
        waits(passed.at[way], leg_recv.at[way])

        def send(d, carry):
            ty = up(y, d, NY)
            remote(
                passed.at[way, ty], gathered.at[source, y], disp_send, disp_recv.at[source], device(y=ty, **along(step))
            ).start()
            return carry

        lax.fori_loop(0, NY, send, 0)

    def shifted(da, db):
        return up(x, da * (1 - c) + db * c, NX), up(y, da * c + db * (1 - c), NY)

    def where_to(tx, ty):
        return ty * (1 - c) + tx * c, tx * (1 - c) + ty * c

    my_b, my_a = where_to(x, y)

    def piece(r, tx, ty):
        return xbuf.at[r, :, :, pl.ds(pl.multiple_of((ty * NX + tx) * LANES, LANES), LANES)]

    def share(r, tx, ty, da, db, step):
        px, py = shifted(da, db)
        remote(piece(r, tx, ty), piece(r, tx, ty), ag_send, ag_recv.at[r, step], device(x=px, y=py)).start()

    def spread(r, direct):
        mine = piece(r, x, y)
        for s in range(NY):
            for h in range(2):
                for p in range(PAIRS):
                    mine[h, pl.ds((s * PAIRS + p) * 2, 2), :] = gathered[r, s, h, p]

        def send_all(p, carry):
            share(r, x, y, lax.rem(p, NX), p // NX, 1)
            return carry

        def send_axes(d, carry):
            share(r, x, y, d, 0, 0)
            share(r, x, y, 0, d, 1)
            return carry

        if direct:
            lax.fori_loop(1, PLANE, send_all, 0)
        else:
            lax.fori_loop(1, NX, send_axes, 0)

    def pass_on(r):
        with scope("wrow"):
            waits(xbuf.at[r, :, :, pl.ds(0, (NX - 1) * LANES)], ag_recv.at[r, 0])

        def take(da, carry):
            tx, ty = shifted(da, 0)
            for db in range(1, NY):
                share(r, tx, ty, 0, db, 1)
            return carry

        lax.fori_loop(1, NX, take, 0)

    def compute(r, direct, direct_sum):
        with scope("wag"):
            waits(xbuf.at[r, :, :, pl.ds(0, (PLANE - 1 if direct else PLANE - NX) * LANES)], ag_recv.at[r, 1])
        up_gate = jnp.dot(xbuf[r, 0], wup[0], preferred_element_type=jnp.float32)
        up_gate = up_gate + jnp.dot(xbuf[r, 1], wup[1], preferred_element_type=jnp.float32)

        def swish(k):
            g, u = up_gate[:, k * 256 : k * 256 + 128], up_gate[:, k * 256 + 128 : k * 256 + 256]
            return (g / (1.0 + jnp.exp(-g)) * u).astype(jnp.bfloat16)

        act = jnp.concatenate([swish(0), swish(1)], axis=1)
        for dy in (2, 1, 3, 0):
            ty = up(y, dy, NY)
            cols = pl.ds(pl.multiple_of(ty * NX * LANES, NX * LANES), NX * LANES)
            for h in range(2):
                out = jnp.dot(act, wdown[h, :, cols], preferred_element_type=jnp.float32).astype(jnp.bfloat16)
                for tx in range(NX):
                    to_b, to_a = where_to(tx, ty)
                    ybuf[r, to_b, to_a, h] = out[:, tx * LANES : (tx + 1) * LANES]
            if not direct_sum:
                continue
            for dx in (2, 1, 3, 0):
                if dx == 0 and dy == 0:
                    continue
                tx = up(x, dx, NX)
                to_b, to_a = where_to(tx, ty)
                remote(
                    ybuf.at[r, to_b, to_a], whole.at[dy * NX + dx - 1], whole_send, whole_recv, device(x=tx, y=ty)
                ).start()
        if not direct_sum:
            for db in (2, 1, 3):
                px, py = shifted(0, db)
                remote(
                    ybuf.at[r, up(my_b, db, NY)], half.at[r, db - 1], half_send, half_recv.at[r], device(x=px, y=py)
                ).start()

    def quarter_sum(r):
        with scope("whalf"):
            waits(half.at[r], half_recv.at[r])
        for da in (2, 1, 3, 0):
            a = up(my_a, da, NX)
            acc = ybuf[r, my_b, a].astype(jnp.float32)
            for k in range(NY - 1):
                acc = acc + half[r, k, a].astype(jnp.float32)
            ybuf[r, my_b, a] = acc.astype(jnp.bfloat16)
            if da:
                px, py = shifted(da, 0)
                remote(
                    ybuf.at[r, my_b, a], quarter.at[r, da - 1], quarter_send, quarter_recv.at[r], device(x=px, y=py)
                ).start()

    def send_home(r, direct_sum):
        acc = ybuf[r, my_b, my_a].astype(jnp.float32)
        if direct_sum:
            with scope("wwhole"):
                waits(whole, whole_recv)
            for s in range(PLANE - 1):
                acc = acc + whole[s].astype(jnp.float32)
        else:
            with scope("wquart"):
                waits(quarter.at[r], quarter_recv.at[r])
            for s in range(NX - 1):
                acc = acc + quarter[r, s].astype(jnp.float32)
        total[...] = acc
        for s in range(NY):
            for h in range(2):
                for p in range(PAIRS):
                    homeward[r, s, h, p] = total[h, pl.ds((s * PAIRS + p) * 2, 2), :].astype(jnp.bfloat16)

        def send(k, carry):
            ty, h = k // 2, lax.rem(k, 2)
            tz = 2 * y + h
            dst = arrived.at[zh, zl]
            here = (r == zh) & (ty == y) & (tz == zl)

            @pl.when(here)
            def _():
                pltpu.make_async_copy(homeward.at[r, ty, h], dst, ret_recv).start()

            @pl.when(jnp.logical_not(here))
            def _():
                remote(homeward.at[r, ty, h], dst, ret_send, ret_recv, device(y=ty, zh=r, zl=tz)).start()
            return carry

        lax.fori_loop(0, 2 * NY, send, 0)

    with scope("wraw"):
        waits(wraw.at[:, pl.ds(0, 2 * UNITS)], load_sem.at[3])
        waits(wdown.at[:, pl.ds(0, UNITS)], load_sem.at[4])
    for h in range(2):
        wup[h, :, pl.ds(0, 256)] = wraw[h, pl.ds(0, 256), :].T

    @pl.when(c == 0)
    def _():
        lax.fori_loop(0, NY, to_region(jnp.where(high, behind, ahead)), 0)

    with scope("wS0"):
        waits(gathered.at[order[0]], disp_recv.at[order[0]])
    with scope("S0"):
        spread(order[0], True)
    @pl.when(c == 1)
    def _():
        lax.fori_loop(0, NY, to_region(ahead), 0)
        lax.fori_loop(0, NY, to_region(behind), 0)
    with scope("R"):
        @pl.when(relays & (zh == 3))
        def _():
            second_leg(1, ahead, -6)

        @pl.when(relays)
        def _():
            second_leg(0, behind, 6)

        @pl.when(relays & (zh != 3))
        def _():
            second_leg(1, ahead, -6)
    for part, _, twin, _ in parts:
        remote(part, twin, twin_send, twin_recv, device(c=1 - c)).start()

    @pl.when(zh == 0)
    def _():
        with scope("wS1"):
            waits(gathered.at[order[1]], disp_recv.at[order[1]])
        with scope("S1"):
            spread(order[1], False)
        with scope("wtwin"):
            waits(wraw.at[:, pl.ds(0, 3 * UNITS)], twin_recv)
        for h in range(2):
            wup[h, :, pl.ds(256, 256)] = wraw[h, pl.ds(256, 256), :].T
        with scope("wS2"):
            waits(gathered.at[order[2]], disp_recv.at[order[2]])
        with scope("S2"):
            spread(order[2], False)
        with scope("A0"):
            compute(work[0], True, False)
        with scope("F1"):
            pass_on(order[1])
        with scope("wS3"):
            waits(gathered.at[order[3]], disp_recv.at[order[3]])
        with scope("S3"):
            spread(order[3], False)
        with scope("F2"):
            pass_on(order[2])
        with scope("A1"):
            compute(work[1], False, False)
        with scope("F3"):
            pass_on(order[3])
        with scope("A2"):
            compute(work[2], False, False)
        with scope("Q0"):
            quarter_sum(work[0])
        with scope("Q1"):
            quarter_sum(work[1])
        with scope("A3"):
            compute(work[3], False, True)
        with scope("Z0"):
            send_home(work[0], False)
        with scope("Q2"):
            quarter_sum(work[2])
        with scope("Z1"):
            send_home(work[1], False)
        with scope("Z2"):
            send_home(work[2], False)
        with scope("Z3"):
            send_home(work[3], True)

    @pl.when(zh == 2)
    def _():
        with scope("wtwin"):
            waits(wraw.at[:, pl.ds(0, 3 * UNITS)], twin_recv)
        for h in range(2):
            wup[h, :, pl.ds(256, 256)] = wraw[h, pl.ds(256, 256), :].T
        with scope("wS2"):
            waits(gathered.at[order[2]], disp_recv.at[order[2]])
        with scope("S2"):
            spread(order[2], True)
        with scope("wS1"):
            waits(gathered.at[order[1]], disp_recv.at[order[1]])
        with scope("S1"):
            spread(order[1], False)
        with scope("A0"):
            compute(work[0], True, True)
        @pl.when(c == 0)
        def _():
            with scope("wS3"):
                waits(gathered.at[order[3]], disp_recv.at[order[3]])
            with scope("S3"):
                spread(order[3], False)

        @pl.when(c == 0)
        def _():
            with scope("F1"):
                pass_on(order[1])

        with scope("Z0"):
            send_home(work[0], True)
        @pl.when(c == 1)
        def _():
            with scope("wS3"):
                waits(gathered.at[order[3]], disp_recv.at[order[3]])
            with scope("S3"):
                spread(order[3], False)

        @pl.when(c == 1)
        def _():
            with scope("F1"):
                pass_on(order[1])

        with scope("F3"):
            pass_on(order[3])
        with scope("A1"):
            compute(work[1], False, False)
        with scope("A3"):
            compute(work[3], False, False)
        with scope("Q1"):
            quarter_sum(work[1])
        with scope("Z1"):
            send_home(work[1], False)
        with scope("A2"):
            compute(work[2], True, False)
        with scope("Q3"):
            quarter_sum(work[3])
        with scope("Z3"):
            send_home(work[3], False)
        with scope("Q2"):
            quarter_sum(work[2])
        with scope("Z2"):
            send_home(work[2], False)

    @pl.when(zh == 1)
    def _():
        with scope("wS1"):
            waits(gathered.at[order[1]], disp_recv.at[order[1]])
        with scope("S1"):
            spread(order[1], True)
        with scope("wtwin"):
            waits(wraw.at[:, pl.ds(0, 3 * UNITS)], twin_recv)
        for h in range(2):
            wup[h, :, pl.ds(256, 256)] = wraw[h, pl.ds(256, 256), :].T
        with scope("A0"):
            compute(work[0], True, False)
        with scope("wS2"):
            waits(gathered.at[order[2]], disp_recv.at[order[2]])
        with scope("S2"):
            spread(order[2], False)
        with scope("F2"):
            pass_on(order[2])
        with scope("A1"):
            compute(work[1], True, True)
        with scope("wS3"):
            waits(gathered.at[order[3]], disp_recv.at[order[3]])
        with scope("S3"):
            spread(order[3], False)
        with scope("Q0"):
            quarter_sum(work[0])
        with scope("A2"):
            compute(work[2], False, False)
        with scope("F3"):
            pass_on(order[3])
        with scope("Z1"):
            send_home(work[1], True)
        with scope("Z0"):
            send_home(work[0], False)
        with scope("A3"):
            compute(work[3], False, False)
        with scope("Q2"):
            quarter_sum(work[2])
        with scope("Z2"):
            send_home(work[2], False)
        with scope("Q3"):
            quarter_sum(work[3])
        with scope("Z3"):
            send_home(work[3], False)

    @pl.when(zh == 3)
    def _():
        with scope("wS1"):
            waits(gathered.at[order[1]], disp_recv.at[order[1]])
        with scope("S1"):
            spread(order[1], False)
        with scope("wtwin"):
            waits(wraw.at[:, pl.ds(0, 3 * UNITS)], twin_recv)
        for h in range(2):
            wup[h, :, pl.ds(256, 256)] = wraw[h, pl.ds(256, 256), :].T
        with scope("A0"):
            compute(work[0], True, False)
        with scope("F1"):
            pass_on(order[1])
        with scope("wS2"):
            waits(gathered.at[order[2]], disp_recv.at[order[2]])
        with scope("S2"):
            spread(order[2], False)
        with scope("F2"):
            pass_on(order[2])
        with scope("A1"):
            compute(work[1], False, False)
        with scope("wS3"):
            waits(gathered.at[order[3]], disp_recv.at[order[3]])
        with scope("S3"):
            spread(order[3], False)
        with scope("Q0"):
            quarter_sum(work[0])
        with scope("A2"):
            compute(work[2], False, False)
        with scope("F3"):
            pass_on(order[3])
        with scope("Q1"):
            quarter_sum(work[1])
        with scope("Z1"):
            send_home(work[1], False)
        with scope("A3"):
            compute(work[3], False, False)
        with scope("Q2"):
            quarter_sum(work[2])
        with scope("Z0"):
            send_home(work[0], False)
        with scope("Z2"):
            send_home(work[2], False)
        with scope("Q3"):
            quarter_sum(work[3])
        with scope("Z3"):
            send_home(work[3], False)

    with scope("wret"):
        waits(arrived, ret_recv)
    for e in range(EXPERTS):
        for p in range(PAIRS):
            part = arrived[0, e, p].astype(jnp.float32)
            for k in range(1, NZH):
                part = part + arrived[k, e, p].astype(jnp.float32)
            returned[pl.ds((e * PAIRS + p) * 2, 2), :] = part
    place = lax.broadcasted_iota(jnp.int32, (EXPERTS * SLOTS, tokens), 0)
    gates = gate_ref[...].astype(jnp.float32)
    combining = jnp.where(n_first == place, gates[0:1, :], 0.0) + jnp.where(n_second == place, gates[1:2, :], 0.0)
    mixed = lax.dot_general(
        combining, returned[...], (((0,), (0,)), ((), ())),
        preferred_element_type=jnp.float32, precision=lax.Precision.HIGHEST,
    )
    residual = hid[:, pl.ds(pl.multiple_of((zl * NX + x) * LANES, LANES), LANES)].astype(jnp.float32)
    out_ref[...] = (residual + mixed).astype(jnp.bfloat16)

    with scope("drain"):
        waits(wraw.at[:, pl.ds(0, 3 * UNITS)], twin_send)
        for _ in range(3):
            waits(gathered.at[1], disp_send)
        waits(gathered.at[0, pl.ds(0, 3)], disp_send)

        @pl.when(relays)
        def _():
            waits(gathered.at[pl.ds(0, 2)], disp_send)

        for r in range(NZH):
            waits(xbuf.at[r, :, :, pl.ds(0, (PLANE - 1) * LANES)], ag_send)
        for r in range(NZH - 1):
            waits(half.at[r], half_send)
            waits(quarter.at[r], quarter_send)

        whole_sum = (zh == 0) | (zh == 1) | (zh == 2)

        @pl.when(jnp.logical_not(whole_sum))
        def _():
            waits(half.at[0], half_send)
            waits(quarter.at[0], quarter_send)

        @pl.when(whole_sum)
        def _():
            waits(whole, whole_send)

        waits(arrived.at[pl.ds(0, 3)], ret_send)
        waits(arrived.at[3, pl.ds(0, 7)], ret_send)

        @pl.when((zl != 2 * y) & (zl != 2 * y + 1))
        def _():
            waits(arrived.at[3, 7], ret_send)


def local(hidden_in, expert_ids, gate_vals, w_gate, w_up, w_down):
    tokens, width = hidden_in.shape
    ids = jnp.swapaxes(expert_ids, 0, 1)
    gates = jnp.swapaxes(gate_vals, 0, 1)
    wg = jnp.swapaxes(w_gate[0], 0, 1)
    wu = jnp.swapaxes(w_up[0], 0, 1)
    bf16, f32 = jnp.bfloat16, jnp.float32
    dma, hbm, vmem = pltpu.SemaphoreType.DMA, pl.BlockSpec(memory_space=pltpu.HBM), pl.BlockSpec(memory_space=pltpu.VMEM)
    return pl.pallas_call(
        moe_kernel,
        name="moe",
        out_shape=jax.ShapeDtypeStruct((tokens, LANES), bf16),
        in_specs=[hbm] * 6,
        out_specs=vmem,
        scratch_shapes=[
            pltpu.VMEM((tokens, width), bf16),
            pltpu.VMEM((2, tokens), jnp.int32),
            pltpu.VMEM((2, tokens), bf16),
            pltpu.VMEM((2, 512, width // 2), bf16),
            pltpu.VMEM((2, width // 2, 512), bf16),
            pltpu.VMEM((2, 256, width // 2), bf16),
            pltpu.VMEM((2, NY, 2, PAIRS, 2, LANES), bf16),
            pltpu.VMEM((2, NY, 2, PAIRS, 2, LANES), bf16),
            pltpu.VMEM((NZH, NY, 2, PAIRS, 2, LANES), bf16),
            pltpu.VMEM((NZH, 2, ROWS, width // 2), bf16),
            pltpu.VMEM((NZH, NY, NX, 2, ROWS, LANES), bf16),
            pltpu.VMEM((NZH, NY - 1, NX, 2, ROWS, LANES), bf16),
            pltpu.VMEM((NZH, NX - 1, 2, ROWS, LANES), bf16),
            pltpu.VMEM((PLANE - 1, 2, ROWS, LANES), bf16),
            pltpu.VMEM((2, ROWS, LANES), f32),
            pltpu.VMEM((NZH, NY, 2, PAIRS, 2, LANES), bf16),
            pltpu.VMEM((NZH, NZL, PAIRS, 2, LANES), bf16),
            pltpu.VMEM((EXPERTS * SLOTS, LANES), f32),
            dma((5,)), dma, dma, dma((2,)), dma, dma((4,)), dma, dma((4, 2)),
            dma, dma((4,)), dma, dma((4,)), dma, dma, dma, dma,
        ],
        compiler_params=pltpu.CompilerParams(
            collective_id=0, has_side_effects=True, vmem_limit_bytes=48 * 1024 * 1024
        ),
    )(*(pltpu.with_memory_space_constraint(a, pltpu.HBM) for a in (hidden_in, ids, gates, wg, wu, w_down[0])))


def solution(mesh):
    split = Mesh(mesh.devices.reshape(NY, NZH, NC, NZL, NX), AXES)
    return jax.shard_map(
        local,
        mesh=split,
        in_specs=(
            P(SEQ, None),
            P(SEQ, None),
            P(SEQ, None),
            P(ET, None, SEQ),
            P(ET, None, SEQ),
            P(ET, SEQ, None),
        ),
        out_specs=P(SEQ, ET),
        check_vma=False,
    )
```

```python
import jax
import jax.numpy as jnp
from jax import lax
from jax.experimental import pallas as pl
from jax.experimental.pallas import tpu as pltpu
from jax.sharding import Mesh
from jax.sharding import PartitionSpec as P

EXPERTS = 8
SLOTS = 10
PAIRS = SLOTS // 2
LANES = 128
AXES = ("y", "zh", "c", "zl", "x")
NY, NZH, NC, NZL, NX = 4, 4, 2, 8, 4
SEQ = ("y", "zh", "c")
ET = ("zl", "x")
ROWS = NY * SLOTS
UNITS = 112
PLANE = NX * NY
MESH = pl.DeviceIdType.MESH


def moe_kernel(
    hidden_any, ids_any, gate_any, wg_any, wu_any, wd_any,
    out_ref,
    hid, ids_ref, gate_ref, wraw, wup, wdown, picked, passed, gathered, xbuf, ybuf, half, quarter, whole, total, homeward, arrived, returned,
    ready, load_sem, twin_send, twin_recv, leg_recv, disp_send, disp_recv, ag_send, ag_recv,
    half_send, half_recv, quarter_send, quarter_recv, whole_send, whole_recv, ret_send, ret_recv,
):
    scope = jax.named_scope
    at = {name: lax.axis_index(name) for name in AXES}
    y, zh, c, zl, x = (at[name] for name in AXES)

    def device(**other):
        return {**at, **other}

    def remote(src, dst, send, recv, dev):
        return pltpu.make_async_remote_copy(
            src_ref=src, dst_ref=dst, send_sem=send, recv_sem=recv, device_id=dev, device_id_type=MESH
        )

    def waits(ref, sem):
        pltpu.make_async_copy(ref, ref, sem).wait()

    def up(v, d, n):
        return lax.rem(v + d, n)

    ahead, behind, across = up(zh, 1, NZH), up(zh, 3, NZH), up(zh, 2, NZH)

    barrier = pltpu.get_barrier_semaphore()

    def hello(**other):
        pl.semaphore_signal(barrier, inc=1, device_id=device(**other), device_id_type=MESH)

    def column(call, target):
        def body(d, carry):
            call(y=up(y, d, NY), zh=target)
            return carry

        lax.fori_loop(0, NY, body, 0)

    high, relays = zl >= NZL // 2, (zl >= 2) & (zl < 6)

    def along(step):
        z = lax.rem(zh * NZL + zl + step + NZH * NZL, NZH * NZL)
        return {"zh": z // NZL, "zl": lax.rem(z, NZL)}

    def hello_relay(d, carry):
        hello(y=up(y, d, NY), **along(jnp.where(high, 6, -6)))
        return carry

    def hello_line(d, carry):
        hello(zl=up(zl, d, NZL))
        return carry

    def hello_plane(p, carry):
        hello(x=up(x, lax.rem(p, NX), NX), y=up(y, p // NX, NY))
        return carry

    @pl.when(zh != 2)
    def _():
        column(hello, ahead)
        column(hello, behind)

    lax.fori_loop(0, NY, hello_relay, 0)

    @pl.when(relays)
    def _():
        hello(**along(6))
        hello(**along(-6))

    lax.fori_loop(1, NZL, hello_line, 0)
    lax.fori_loop(1, PLANE, hello_plane, 0)
    hello(c=1 - c)

    width = wdown.shape[2]
    small = [
        pltpu.make_async_copy(ids_any, ids_ref, load_sem.at[0]),
        pltpu.make_async_copy(gate_any, gate_ref, load_sem.at[1]),
        pltpu.make_async_copy(hidden_any, hid, load_sem.at[2]),
    ]
    parts = []
    for h in range(2):
        for ty in range(NY):
            cols, to = pl.ds((2 * ty + h) * NX * LANES, NX * LANES), pl.ds(ty * NX * LANES, NX * LANES)
            for k, (weight, buf, own, twin) in enumerate(
                ((wg_any, wraw, 0, 256), (wu_any, wraw, 128, 384), (wd_any, wdown, 0, 128))
            ):
                parts.append((
                    weight.at[:, cols], buf.at[h, pl.ds(own, UNITS), to], buf.at[h, pl.ds(twin, UNITS), to], 3 + k // 2
                ))
    loads = [pltpu.make_async_copy(part, own, load_sem.at[sem]) for part, own, _, sem in parts]
    for load in small + loads:
        load.start()
    blank = jnp.zeros((128 - UNITS, width), jnp.bfloat16)
    for h in range(2):
        for k in range(4):
            wraw[h, pl.ds(k * 128 + UNITS, 128 - UNITS), :] = blank
        for k in range(2):
            wdown[h, pl.ds(k * 128 + UNITS, 128 - UNITS), :] = blank
    small[0].wait()
    small[1].wait()

    tokens = ids_ref.shape[1]
    ids = ids_ref[...]
    expert = lax.broadcasted_iota(jnp.int32, (EXPERTS, tokens), 0)
    first, second = ids[0:1, :], ids[1:2, :]
    named = (jnp.where(first == expert, 1.0, 0.0) + jnp.where(second == expert, 1.0, 0.0)).astype(jnp.float32)
    before = jnp.where(
        lax.broadcasted_iota(jnp.int32, (tokens, tokens), 0) < lax.broadcasted_iota(jnp.int32, (tokens, tokens), 1),
        1.0, 0.0,
    ).astype(jnp.float32)
    earlier = jnp.dot(named, before, preferred_element_type=jnp.float32)

    def number(chosen):
        slot = jnp.sum(jnp.where(chosen == expert, earlier, 0.0), axis=0, keepdims=True)
        return chosen * SLOTS + slot.astype(jnp.int32)

    n_first, n_second = number(first), number(second)
    slot = lax.broadcasted_iota(jnp.int32, (16, tokens), 0)

    def placing(expert_here):
        wanted = jnp.where(slot < SLOTS, slot + expert_here * SLOTS, -1)
        return (
            jnp.where(n_first == wanted, 1.0, 0.0) + jnp.where(n_second == wanted, 1.0, 0.0)
        ).astype(jnp.bfloat16)

    places = jnp.concatenate([placing(zl), placing(lax.rem(zl + NZL // 2, NZL))], axis=0)
    small[2].wait()
    for j in range(NZL):
        block = hid[:, pl.ds(pl.multiple_of((j * NX + x) * LANES, LANES), LANES)]
        rows = jnp.dot(places, block, preferred_element_type=jnp.float32)
        for k in range(2):
            for p in range(PAIRS):
                picked[k, j // 2, j % 2, p] = rows[16 * k + 2 * p : 16 * k + 2 * p + 2].astype(jnp.bfloat16)

    with scope("w_barrier"):
        pl.semaphore_wait(barrier, jnp.where(lax.rem(zh, 2) == 0, 2 * NY, NY) + (NZL - 1) + (PLANE - 1) + 2 + jnp.where(relays, 2 * NY, 0))

    order = (
        jnp.where(zh == 0, 0, jnp.where(zh == 1, 1, jnp.where(zh == 2, 2, 3))),
        jnp.where(zh == 0, 1, jnp.where(zh == 1, 0, jnp.where(zh == 2, 1, 0))),
        jnp.where(zh == 0, 3, jnp.where(zh == 1, 2, jnp.where(zh == 2, 0, 1))),
        jnp.where(zh == 0, 2, jnp.where(zh == 1, 3, jnp.where(zh == 2, 3, 2))),
    )
    work = (
        jnp.where(zh == 0, 0, jnp.where(zh == 1, 1, jnp.where(zh == 2, 0, 3))),
        jnp.where(zh == 0, 1, jnp.where(zh == 1, 0, jnp.where(zh == 2, 1, 0))),
        jnp.where(zh == 0, 3, jnp.where(zh == 1, 2, jnp.where(zh == 2, 2, 1))),
        jnp.where(zh == 0, 2, jnp.where(zh == 1, 3, jnp.where(zh == 2, 3, 2))),
    )

    def say_ready(**other):
        pl.semaphore_signal(ready, inc=1, device_id=device(**other), device_id_type=MESH)

    @pl.when(zh == 2)
    def _():
        column(say_ready, ahead)
        column(say_ready, behind)

    @pl.when(high)
    def _():
        remote(picked.at[1], passed.at[0], disp_send, leg_recv.at[0], device(**along(6))).start()

    @pl.when(jnp.logical_not(high))
    def _():
        remote(picked.at[1], passed.at[1], disp_send, leg_recv.at[1], device(**along(-6))).start()

    def to_region(target):
        def send(d, carry):
            ty = up(y, d, NY)
            remote(
                picked.at[0, ty], gathered.at[zh, y], disp_send, disp_recv.at[zh], device(y=ty, zh=target)
            ).start()
            return carry
        return send

    lax.fori_loop(1, NY, to_region(zh), 0)
    pltpu.make_async_copy(picked.at[0, y], gathered.at[zh, y], disp_recv.at[zh]).start()

    def second_leg(way, source, step):
        with scope("leg"):
            waits(passed.at[way], leg_recv.at[way])

        def send(d, carry):
            ty = up(y, d, NY)
            remote(
                passed.at[way, ty], gathered.at[source, y], disp_send, disp_recv.at[source], device(y=ty, **along(step))
            ).start()
            return carry

        lax.fori_loop(0, NY, send, 0)

    def shifted(da, db):
        return up(x, da * (1 - c) + db * c, NX), up(y, da * c + db * (1 - c), NY)

    def where_to(tx, ty):
        return ty * (1 - c) + tx * c, tx * (1 - c) + ty * c

    my_b, my_a = where_to(x, y)

    def piece(r, tx, ty):
        return xbuf.at[r, :, :, pl.ds(pl.multiple_of((ty * NX + tx) * LANES, LANES), LANES)]

    def share(r, tx, ty, da, db, step):
        px, py = shifted(da, db)
        remote(piece(r, tx, ty), piece(r, tx, ty), ag_send, ag_recv.at[r, step], device(x=px, y=py)).start()

    def spread(r, direct):
        mine = piece(r, x, y)
        for s in range(NY):
            for h in range(2):
                for p in range(PAIRS):
                    mine[h, pl.ds((s * PAIRS + p) * 2, 2), :] = gathered[r, s, h, p]

        def send_all(p, carry):
            px, py = up(x, lax.rem(p, NX), NX), up(y, p // NX, NY)
            remote(mine, mine, ag_send, ag_recv.at[r, 2 + p // NX], device(x=px, y=py)).start()
            return carry

        def send_axes(d, carry):
            share(r, x, y, d, 0, 0)
            share(r, x, y, 0, d, 1)
            return carry

        if direct:
            lax.fori_loop(1, PLANE, send_all, 0)
        else:
            lax.fori_loop(1, NX, send_axes, 0)

    def pass_on(r):
        with scope("wrow"):
            waits(xbuf.at[r, :, :, pl.ds(0, (NX - 1) * LANES)], ag_recv.at[r, 0])

        def take(da, carry):
            tx, ty = shifted(da, 0)
            for db in range(1, NY):
                share(r, tx, ty, 0, db, 1)
            return carry

        lax.fori_loop(1, NX, take, 0)

    def halve(r):
        for db in (2, 1, 3):
            px, py = shifted(0, db)
            remote(
                ybuf.at[r, up(my_b, db, NY)], half.at[r, db - 1], half_send, half_recv.at[r], device(x=px, y=py)
            ).start()

    def compute(r, direct, direct_sum, hold=False):
        if direct:
            up_gate = None
            for dy in (0, 1, 3, 2):
                with scope("wag"):
                    waits(xbuf.at[r, :, :, pl.ds(0, (NX if dy else NX - 1) * LANES)], ag_recv.at[r, 2 + dy])
                row = pl.ds(pl.multiple_of(up(y, NY - dy, NY) * NX * LANES, NX * LANES), NX * LANES)
                for h in range(2):
                    part = jnp.dot(xbuf[r, h, :, row], wup[h, row, :], preferred_element_type=jnp.float32)
                    up_gate = part if up_gate is None else up_gate + part
        else:
            with scope("wag"):
                waits(xbuf.at[r, :, :, pl.ds(0, (PLANE - NX) * LANES)], ag_recv.at[r, 1])
            up_gate = jnp.dot(xbuf[r, 0], wup[0], preferred_element_type=jnp.float32)
            up_gate = up_gate + jnp.dot(xbuf[r, 1], wup[1], preferred_element_type=jnp.float32)

        def swish(k):
            g, u = up_gate[:, k * 256 : k * 256 + 128], up_gate[:, k * 256 + 128 : k * 256 + 256]
            return (g / (1.0 + jnp.exp(-g)) * u).astype(jnp.bfloat16)

        act = jnp.concatenate([swish(0), swish(1)], axis=1)
        for dy in (2, 1, 3, 0):
            ty = up(y, dy, NY)
            cols = pl.ds(pl.multiple_of(ty * NX * LANES, NX * LANES), NX * LANES)
            for h in range(2):
                out = jnp.dot(act, wdown[h, :, cols], preferred_element_type=jnp.float32).astype(jnp.bfloat16)
                for tx in range(NX):
                    to_b, to_a = where_to(tx, ty)
                    ybuf[r, to_b, to_a, h] = out[:, tx * LANES : (tx + 1) * LANES]
            if not direct_sum:
                continue
            for dx in (2, 1, 3, 0):
                if dx == 0 and dy == 0:
                    continue
                tx = up(x, dx, NX)
                to_b, to_a = where_to(tx, ty)
                remote(
                    ybuf.at[r, to_b, to_a], whole.at[dy * NX + dx - 1], whole_send, whole_recv, device(x=tx, y=ty)
                ).start()
        if not direct_sum and not hold:
            halve(r)

    def quarter_sum(r):
        with scope("whalf"):
            waits(half.at[r], half_recv.at[r])
        for da in (2, 1, 3, 0):
            a = up(my_a, da, NX)
            acc = ybuf[r, my_b, a].astype(jnp.float32)
            for k in range(NY - 1):
                acc = acc + half[r, k, a].astype(jnp.float32)
            ybuf[r, my_b, a] = acc.astype(jnp.bfloat16)
            if da:
                px, py = shifted(da, 0)
                remote(
                    ybuf.at[r, my_b, a], quarter.at[r, da - 1], quarter_send, quarter_recv.at[r], device(x=px, y=py)
                ).start()

    def send_home(r, direct_sum):
        acc = ybuf[r, my_b, my_a].astype(jnp.float32)
        if direct_sum:
            with scope("wwhole"):
                waits(whole, whole_recv)
            for s in range(PLANE - 1):
                acc = acc + whole[s].astype(jnp.float32)
        else:
            with scope("wquart"):
                waits(quarter.at[r], quarter_recv.at[r])
            for s in range(NX - 1):
                acc = acc + quarter[r, s].astype(jnp.float32)
        total[...] = acc
        for s in range(NY):
            for h in range(2):
                for p in range(PAIRS):
                    homeward[r, s, h, p] = total[h, pl.ds((s * PAIRS + p) * 2, 2), :].astype(jnp.bfloat16)

        def send(k, carry):
            ty, h = k // 2, lax.rem(k, 2)
            tz = 2 * y + h
            dst = arrived.at[zh, zl]
            here = (r == zh) & (ty == y) & (tz == zl)

            @pl.when(here)
            def _():
                pltpu.make_async_copy(homeward.at[r, ty, h], dst, ret_recv).start()

            @pl.when(jnp.logical_not(here))
            def _():
                remote(homeward.at[r, ty, h], dst, ret_send, ret_recv, device(y=ty, zh=r, zl=tz)).start()
            return carry

        lax.fori_loop(0, 2 * NY, send, 0)

    with scope("wraw"):
        waits(wraw.at[:, pl.ds(0, 2 * UNITS)], load_sem.at[3])
        waits(wdown.at[:, pl.ds(0, UNITS)], load_sem.at[4])
    for h in range(2):
        wup[h, :, pl.ds(0, 256)] = wraw[h, pl.ds(0, 256), :].T

    @pl.when((c == 0) & (lax.rem(zh, 2) == 0))
    def _():
        lax.fori_loop(0, NY, to_region(jnp.where(high, ahead, behind)), 0)

    @pl.when((c == 0) & (lax.rem(zh, 2) == 0))
    def _():
        lax.fori_loop(0, NY, to_region(jnp.where(high, behind, ahead)), 0)

    @pl.when((c == 0) & (lax.rem(zh, 2) == 1))
    def _():
        lax.fori_loop(0, NY, to_region(0), 0)

    with scope("wS0"):
        waits(gathered.at[order[0]], disp_recv.at[order[0]])
    with scope("S0"):
        spread(order[0], True)
    @pl.when(c == 1)
    def _():
        lax.fori_loop(0, NY, to_region(jnp.where(lax.rem(zh, 2) == 0, ahead, 0)), 0)

        @pl.when(lax.rem(zh, 2) == 0)
        def _():
            lax.fori_loop(0, NY, to_region(behind), 0)

    with scope("R"):
        @pl.when(relays & (zh == 3))
        def _():
            second_leg(1, ahead, -6)

        @pl.when(relays)
        def _():
            second_leg(0, behind, 6)

        @pl.when(relays & (zh != 3))
        def _():
            second_leg(1, ahead, -6)
    for part, _, twin, _ in parts:
        remote(part, twin, twin_send, twin_recv, device(c=1 - c)).start()

    @pl.when(zh == 0)
    def _():
        with scope("wS1"):
            waits(gathered.at[order[1]], disp_recv.at[order[1]])
        with scope("S1"):
            spread(order[1], False)
        with scope("wtwin"):
            waits(wraw.at[:, pl.ds(0, 3 * UNITS)], twin_recv)
        for h in range(2):
            wup[h, :, pl.ds(256, 256)] = wraw[h, pl.ds(256, 256), :].T
        with scope("wS2"):
            waits(gathered.at[order[2]], disp_recv.at[order[2]])
        with scope("S2"):
            spread(order[2], False)
        with scope("A0"):
            compute(work[0], True, False)
        with scope("F1"):
            pass_on(order[1])
        with scope("wS3"):
            waits(gathered.at[order[3]], disp_recv.at[order[3]])
        with scope("S3"):
            spread(order[3], False)
        with scope("F2"):
            pass_on(order[2])
        with scope("A1"):
            compute(work[1], False, False)
        with scope("F3"):
            pass_on(order[3])
        with scope("A2"):
            compute(work[2], False, False)
        with scope("Q0"):
            quarter_sum(work[0])
        with scope("Q1"):
            quarter_sum(work[1])
        with scope("A3"):
            compute(work[3], False, True)
        with scope("Z0"):
            send_home(work[0], False)
        with scope("Q2"):
            quarter_sum(work[2])
        with scope("Z1"):
            send_home(work[1], False)
        with scope("Z2"):
            send_home(work[2], False)
        with scope("Z3"):
            send_home(work[3], True)

    @pl.when(zh == 2)
    def _():
        with scope("wtwin"):
            waits(wraw.at[:, pl.ds(0, 3 * UNITS)], twin_recv)
        for h in range(2):
            wup[h, :, pl.ds(256, 256)] = wraw[h, pl.ds(256, 256), :].T
        with scope("wS2"):
            waits(gathered.at[order[2]], disp_recv.at[order[2]])
        with scope("S2"):
            spread(order[2], True)
        with scope("wS1"):
            waits(gathered.at[order[1]], disp_recv.at[order[1]])
        with scope("S1"):
            spread(order[1], False)
        with scope("A0"):
            compute(work[0], True, True)
        @pl.when(c == 0)
        def _():
            with scope("wS3"):
                waits(gathered.at[order[3]], disp_recv.at[order[3]])
            with scope("S3"):
                spread(order[3], False)

        with scope("F1"):
            pass_on(order[1])
        with scope("A2"):
            compute(work[2], True, False, True)
        with scope("Z0"):
            send_home(work[0], True)
        @pl.when(c == 1)
        def _():
            with scope("wS3"):
                waits(gathered.at[order[3]], disp_recv.at[order[3]])
            with scope("S3"):
                spread(order[3], False)

        @pl.when(c == 0)
        def _():
            with scope("F3"):
                pass_on(order[3])

        with scope("A1"):
            compute(work[1], False, False)
        @pl.when(c == 1)
        def _():
            with scope("F3"):
                pass_on(order[3])

        @pl.when(c == 0)
        def _():
            with scope("A3"):
                compute(work[3], False, False)

        with scope("H2"):
            halve(work[2])
        with scope("Q1"):
            quarter_sum(work[1])
        @pl.when(c == 1)
        def _():
            with scope("A3"):
                compute(work[3], False, False)

        with scope("Z1"):
            send_home(work[1], False)
        with scope("Q3"):
            quarter_sum(work[3])
        with scope("Q2"):
            quarter_sum(work[2])
        with scope("Z3"):
            send_home(work[3], False)
        with scope("Z2"):
            send_home(work[2], False)

    @pl.when(zh == 1)
    def _():
        with scope("wS1"):
            waits(gathered.at[order[1]], disp_recv.at[order[1]])
        with scope("S1"):
            spread(order[1], True)
        with scope("NL"):
            pl.semaphore_wait(ready, NY)
        lax.fori_loop(0, NY, to_region(2), 0)
        with scope("wtwin"):
            waits(wraw.at[:, pl.ds(0, 3 * UNITS)], twin_recv)
        for h in range(2):
            wup[h, :, pl.ds(256, 256)] = wraw[h, pl.ds(256, 256), :].T
        with scope("A0"):
            compute(work[0], True, False)
        with scope("wS2"):
            waits(gathered.at[order[2]], disp_recv.at[order[2]])
        with scope("S2"):
            spread(order[2], False)
        with scope("wS3"):
            waits(gathered.at[order[3]], disp_recv.at[order[3]])
        with scope("S3"):
            spread(order[3], False)
        with scope("F2"):
            pass_on(order[2])
        with scope("A1"):
            compute(work[1], True, True)
        with scope("F3"):
            pass_on(order[3])
        with scope("Q0"):
            quarter_sum(work[0])
        with scope("A2"):
            compute(work[2], False, False)
        with scope("Z1"):
            send_home(work[1], True)
        with scope("Z0"):
            send_home(work[0], False)
        with scope("A3"):
            compute(work[3], False, False)
        with scope("Q2"):
            quarter_sum(work[2])
        with scope("Z2"):
            send_home(work[2], False)
        with scope("Q3"):
            quarter_sum(work[3])
        with scope("Z3"):
            send_home(work[3], False)

    @pl.when(zh == 3)
    def _():
        with scope("wS1"):
            waits(gathered.at[order[1]], disp_recv.at[order[1]])
        with scope("S1"):
            spread(order[1], False)
        with scope("NL"):
            pl.semaphore_wait(ready, NY)
        lax.fori_loop(0, NY, to_region(2), 0)
        with scope("wtwin"):
            waits(wraw.at[:, pl.ds(0, 3 * UNITS)], twin_recv)
        for h in range(2):
            wup[h, :, pl.ds(256, 256)] = wraw[h, pl.ds(256, 256), :].T
        with scope("A0"):
            compute(work[0], True, False)
        with scope("F1"):
            pass_on(order[1])
        with scope("wS2"):
            waits(gathered.at[order[2]], disp_recv.at[order[2]])
        with scope("S2"):
            spread(order[2], False)
        with scope("F2"):
            pass_on(order[2])
        with scope("A1"):
            compute(work[1], False, False)
        with scope("wS3"):
            waits(gathered.at[order[3]], disp_recv.at[order[3]])
        with scope("S3"):
            spread(order[3], False)
        with scope("Q0"):
            quarter_sum(work[0])
        with scope("A2"):
            compute(work[2], False, False)
        with scope("F3"):
            pass_on(order[3])
        with scope("Q1"):
            quarter_sum(work[1])
        with scope("Z1"):
            send_home(work[1], False)
        with scope("A3"):
            compute(work[3], False, False)
        with scope("Q2"):
            quarter_sum(work[2])
        with scope("Z0"):
            send_home(work[0], False)
        with scope("Z2"):
            send_home(work[2], False)
        with scope("Q3"):
            quarter_sum(work[3])
        with scope("Z3"):
            send_home(work[3], False)

    with scope("wret"):
        waits(arrived, ret_recv)
    for e in range(EXPERTS):
        for p in range(PAIRS):
            part = arrived[0, e, p].astype(jnp.float32)
            for k in range(1, NZH):
                part = part + arrived[k, e, p].astype(jnp.float32)
            returned[pl.ds((e * PAIRS + p) * 2, 2), :] = part
    place = lax.broadcasted_iota(jnp.int32, (EXPERTS * SLOTS, tokens), 0)
    gates = gate_ref[...].astype(jnp.float32)
    combining = jnp.where(n_first == place, gates[0:1, :], 0.0) + jnp.where(n_second == place, gates[1:2, :], 0.0)
    mixed = lax.dot_general(
        combining, returned[...], (((0,), (0,)), ((), ())),
        preferred_element_type=jnp.float32, precision=lax.Precision.HIGHEST,
    )
    residual = hid[:, pl.ds(pl.multiple_of((zl * NX + x) * LANES, LANES), LANES)].astype(jnp.float32)
    out_ref[...] = (residual + mixed).astype(jnp.bfloat16)

    with scope("drain"):
        waits(wraw.at[:, pl.ds(0, 3 * UNITS)], twin_send)
        for _ in range(3):
            waits(gathered.at[1], disp_send)
        waits(gathered.at[0, pl.ds(0, 3)], disp_send)

        @pl.when(relays)
        def _():
            waits(gathered.at[pl.ds(0, 2)], disp_send)

        for r in range(NZH):
            waits(xbuf.at[r, :, :, pl.ds(0, (PLANE - 1) * LANES)], ag_send)
        for r in range(NZH - 1):
            waits(half.at[r], half_send)
            waits(quarter.at[r], quarter_send)

        whole_sum = (zh == 0) | (zh == 1) | (zh == 2)

        @pl.when(jnp.logical_not(whole_sum))
        def _():
            waits(half.at[0], half_send)
            waits(quarter.at[0], quarter_send)

        @pl.when(whole_sum)
        def _():
            waits(whole, whole_send)

        waits(arrived.at[pl.ds(0, 3)], ret_send)
        waits(arrived.at[3, pl.ds(0, 7)], ret_send)

        @pl.when((zl != 2 * y) & (zl != 2 * y + 1))
        def _():
            waits(arrived.at[3, 7], ret_send)


def local(hidden_in, expert_ids, gate_vals, w_gate, w_up, w_down):
    tokens, width = hidden_in.shape
    ids = jnp.swapaxes(expert_ids, 0, 1)
    gates = jnp.swapaxes(gate_vals, 0, 1)
    wg = jnp.swapaxes(w_gate[0], 0, 1)
    wu = jnp.swapaxes(w_up[0], 0, 1)
    bf16, f32 = jnp.bfloat16, jnp.float32
    dma, hbm, vmem = pltpu.SemaphoreType.DMA, pl.BlockSpec(memory_space=pltpu.HBM), pl.BlockSpec(memory_space=pltpu.VMEM)
    return pl.pallas_call(
        moe_kernel,
        name="moe",
        out_shape=jax.ShapeDtypeStruct((tokens, LANES), bf16),
        in_specs=[hbm] * 6,
        out_specs=vmem,
        scratch_shapes=[
            pltpu.VMEM((tokens, width), bf16),
            pltpu.VMEM((2, tokens), jnp.int32),
            pltpu.VMEM((2, tokens), bf16),
            pltpu.VMEM((2, 512, width // 2), bf16),
            pltpu.VMEM((2, width // 2, 512), bf16),
            pltpu.VMEM((2, 256, width // 2), bf16),
            pltpu.VMEM((2, NY, 2, PAIRS, 2, LANES), bf16),
            pltpu.VMEM((2, NY, 2, PAIRS, 2, LANES), bf16),
            pltpu.VMEM((NZH, NY, 2, PAIRS, 2, LANES), bf16),
            pltpu.VMEM((NZH, 2, ROWS, width // 2), bf16),
            pltpu.VMEM((NZH, NY, NX, 2, ROWS, LANES), bf16),
            pltpu.VMEM((NZH, NY - 1, NX, 2, ROWS, LANES), bf16),
            pltpu.VMEM((NZH, NX - 1, 2, ROWS, LANES), bf16),
            pltpu.VMEM((PLANE - 1, 2, ROWS, LANES), bf16),
            pltpu.VMEM((2, ROWS, LANES), f32),
            pltpu.VMEM((NZH, NY, 2, PAIRS, 2, LANES), bf16),
            pltpu.VMEM((NZH, NZL, PAIRS, 2, LANES), bf16),
            pltpu.VMEM((EXPERTS * SLOTS, LANES), f32),
            pltpu.SemaphoreType.REGULAR, dma((5,)), dma, dma, dma((2,)), dma, dma((4,)), dma, dma((4, 2 + NY)),
            dma, dma((4,)), dma, dma((4,)), dma, dma, dma, dma,
        ],
        compiler_params=pltpu.CompilerParams(
            collective_id=0, has_side_effects=True, vmem_limit_bytes=48 * 1024 * 1024
        ),
    )(*(pltpu.with_memory_space_constraint(a, pltpu.HBM) for a in (hidden_in, ids, gates, wg, wu, w_down[0])))


def solution(mesh):
    split = Mesh(mesh.devices.reshape(NY, NZH, NC, NZL, NX), AXES)
    return jax.shard_map(
        local,
        mesh=split,
        in_specs=(
            P(SEQ, None),
            P(SEQ, None),
            P(SEQ, None),
            P(ET, None, SEQ),
            P(ET, None, SEQ),
            P(ET, SEQ, None),
        ),
        out_specs=P(SEQ, ET),
        check_vma=False,
    )
```

```python
import jax
import jax.numpy as jnp
from jax import lax
from jax.experimental import pallas as pl
from jax.experimental.pallas import tpu as pltpu
from jax.sharding import Mesh
from jax.sharding import PartitionSpec as P

EXPERTS = 8
SLOTS = 10
PAIRS = SLOTS // 2
LANES = 128
AXES = ("y", "zh", "c", "zl", "x")
NY, NZH, NC, NZL, NX = 4, 4, 2, 8, 4
SEQ = ("y", "zh", "c")
ET = ("zl", "x")
ROWS = NY * SLOTS
UNITS = 112
PLANE = NX * NY
MESH = pl.DeviceIdType.MESH


def moe_kernel(
    hidden_any, ids_any, gate_any, wg_any, wu_any, wd_any,
    out_ref,
    hid, ids_ref, gate_ref, wraw, wup, wdown, picked, passed, gathered, xbuf, ybuf, half, quarter, whole, total, homeward, arrived, returned,
    ready, load_sem, twin_send, twin_recv, leg_recv, disp_send, disp_recv, ag_send, ag_recv,
    half_send, half_recv, quarter_send, quarter_recv, whole_send, whole_recv, ret_send, ret_recv,
):
    scope = jax.named_scope
    at = {name: lax.axis_index(name) for name in AXES}
    y, zh, c, zl, x = (at[name] for name in AXES)

    def device(**other):
        return {**at, **other}

    def remote(src, dst, send, recv, dev):
        return pltpu.make_async_remote_copy(
            src_ref=src, dst_ref=dst, send_sem=send, recv_sem=recv, device_id=dev, device_id_type=MESH
        )

    def waits(ref, sem):
        pltpu.make_async_copy(ref, ref, sem).wait()

    def up(v, d, n):
        return lax.rem(v + d, n)

    ahead, behind, across = up(zh, 1, NZH), up(zh, 3, NZH), up(zh, 2, NZH)

    barrier = pltpu.get_barrier_semaphore()

    def hello(**other):
        pl.semaphore_signal(barrier, inc=1, device_id=device(**other), device_id_type=MESH)

    def column(call, target):
        def body(d, carry):
            call(y=up(y, d, NY), zh=target)
            return carry

        lax.fori_loop(0, NY, body, 0)

    high, relays = zl >= NZL // 2, (zl >= 2) & (zl < 6)

    def along(step):
        z = lax.rem(zh * NZL + zl + step + NZH * NZL, NZH * NZL)
        return {"zh": z // NZL, "zl": lax.rem(z, NZL)}

    def hello_relay(d, carry):
        hello(y=up(y, d, NY), **along(jnp.where(high, 6, -6)))
        return carry

    def hello_line(d, carry):
        hello(zl=up(zl, d, NZL))
        return carry

    def hello_plane(p, carry):
        hello(x=up(x, lax.rem(p, NX), NX), y=up(y, p // NX, NY))
        return carry

    @pl.when(zh != 2)
    def _():
        column(hello, ahead)
        column(hello, behind)

    lax.fori_loop(0, NY, hello_relay, 0)

    @pl.when(relays)
    def _():
        hello(**along(6))
        hello(**along(-6))

    lax.fori_loop(1, NZL, hello_line, 0)
    lax.fori_loop(1, PLANE, hello_plane, 0)
    hello(c=1 - c)

    width = wdown.shape[2]
    small = [
        pltpu.make_async_copy(ids_any, ids_ref, load_sem.at[0]),
        pltpu.make_async_copy(gate_any, gate_ref, load_sem.at[1]),
        pltpu.make_async_copy(hidden_any, hid, load_sem.at[2]),
    ]
    parts = []
    for h in range(2):
        for ty in range(NY):
            cols, to = pl.ds((2 * ty + h) * NX * LANES, NX * LANES), pl.ds(ty * NX * LANES, NX * LANES)
            for k, (weight, buf, own, twin) in enumerate(
                ((wg_any, wraw, 0, 256), (wu_any, wraw, 128, 384), (wd_any, wdown, 0, 128))
            ):
                parts.append((
                    weight.at[:, cols], buf.at[h, pl.ds(own, UNITS), to], buf.at[h, pl.ds(twin, UNITS), to], 3 + k // 2
                ))
    loads = [pltpu.make_async_copy(part, own, load_sem.at[sem]) for part, own, _, sem in parts]
    for load in small + loads:
        load.start()
    blank = jnp.zeros((128 - UNITS, width), jnp.bfloat16)
    for h in range(2):
        for k in range(4):
            wraw[h, pl.ds(k * 128 + UNITS, 128 - UNITS), :] = blank
        for k in range(2):
            wdown[h, pl.ds(k * 128 + UNITS, 128 - UNITS), :] = blank
    small[0].wait()
    small[1].wait()

    tokens = ids_ref.shape[1]
    ids = ids_ref[...]
    expert = lax.broadcasted_iota(jnp.int32, (EXPERTS, tokens), 0)
    first, second = ids[0:1, :], ids[1:2, :]
    named = (jnp.where(first == expert, 1.0, 0.0) + jnp.where(second == expert, 1.0, 0.0)).astype(jnp.float32)
    before = jnp.where(
        lax.broadcasted_iota(jnp.int32, (tokens, tokens), 0) < lax.broadcasted_iota(jnp.int32, (tokens, tokens), 1),
        1.0, 0.0,
    ).astype(jnp.float32)
    earlier = jnp.dot(named, before, preferred_element_type=jnp.float32)

    def number(chosen):
        slot = jnp.sum(jnp.where(chosen == expert, earlier, 0.0), axis=0, keepdims=True)
        return chosen * SLOTS + slot.astype(jnp.int32)

    n_first, n_second = number(first), number(second)
    slot = lax.broadcasted_iota(jnp.int32, (16, tokens), 0)

    def placing(expert_here):
        wanted = jnp.where(slot < SLOTS, slot + expert_here * SLOTS, -1)
        return (
            jnp.where(n_first == wanted, 1.0, 0.0) + jnp.where(n_second == wanted, 1.0, 0.0)
        ).astype(jnp.bfloat16)

    places = jnp.concatenate([placing(zl), placing(lax.rem(zl + NZL // 2, NZL))], axis=0)
    small[2].wait()
    for j in range(NZL):
        block = hid[:, pl.ds(pl.multiple_of((j * NX + x) * LANES, LANES), LANES)]
        rows = jnp.dot(places, block, preferred_element_type=jnp.float32)
        for k in range(2):
            for p in range(PAIRS):
                picked[k, j // 2, j % 2, p] = rows[16 * k + 2 * p : 16 * k + 2 * p + 2].astype(jnp.bfloat16)

    with scope("w_barrier"):
        pl.semaphore_wait(barrier, jnp.where(lax.rem(zh, 2) == 0, 2 * NY, NY) + (NZL - 1) + (PLANE - 1) + 2 + jnp.where(relays, 2 * NY, 0))

    order = (
        jnp.where(zh == 0, 0, jnp.where(zh == 1, 1, jnp.where(zh == 2, 2, 3))),
        jnp.where(zh == 0, 1, jnp.where(zh == 1, 0, jnp.where(zh == 2, 1, 0))),
        jnp.where(zh == 0, 3, jnp.where(zh == 1, 2, jnp.where(zh == 2, 0, 1))),
        jnp.where(zh == 0, 2, jnp.where(zh == 1, 3, jnp.where(zh == 2, 3, 2))),
    )
    work = (
        jnp.where(zh == 0, 0, jnp.where(zh == 1, 1, jnp.where(zh == 2, 0, 3))),
        jnp.where(zh == 0, 1, jnp.where(zh == 1, 0, jnp.where(zh == 2, 1, 0))),
        jnp.where(zh == 0, 3, jnp.where(zh == 1, 2, jnp.where(zh == 2, 2, 1))),
        jnp.where(zh == 0, 2, jnp.where(zh == 1, 3, jnp.where(zh == 2, 3, 2))),
    )

    def say_ready(**other):
        pl.semaphore_signal(ready, inc=1, device_id=device(**other), device_id_type=MESH)

    @pl.when(zh == 2)
    def _():
        column(say_ready, ahead)
        column(say_ready, behind)

    @pl.when(high)
    def _():
        remote(picked.at[1], passed.at[0], disp_send, leg_recv.at[0], device(**along(6))).start()

    @pl.when(jnp.logical_not(high))
    def _():
        remote(picked.at[1], passed.at[1], disp_send, leg_recv.at[1], device(**along(-6))).start()

    def to_region(target):
        def send(d, carry):
            ty = up(y, d, NY)
            remote(
                picked.at[0, ty], gathered.at[zh, y], disp_send, disp_recv.at[zh], device(y=ty, zh=target)
            ).start()
            return carry
        return send

    lax.fori_loop(1, NY, to_region(zh), 0)
    pltpu.make_async_copy(picked.at[0, y], gathered.at[zh, y], disp_recv.at[zh]).start()

    def second_leg(way, source, step):
        with scope("leg"):
            waits(passed.at[way], leg_recv.at[way])

        def send(d, carry):
            ty = up(y, d, NY)
            remote(
                passed.at[way, ty], gathered.at[source, y], disp_send, disp_recv.at[source], device(y=ty, **along(step))
            ).start()
            return carry

        lax.fori_loop(0, NY, send, 0)

    def shifted(da, db):
        return up(x, da * (1 - c) + db * c, NX), up(y, da * c + db * (1 - c), NY)

    def where_to(tx, ty):
        return ty * (1 - c) + tx * c, tx * (1 - c) + ty * c

    my_b, my_a = where_to(x, y)

    def piece(r, tx, ty):
        return xbuf.at[r, :, :, pl.ds(pl.multiple_of((ty * NX + tx) * LANES, LANES), LANES)]

    def share(r, tx, ty, da, db, step):
        px, py = shifted(da, db)
        remote(piece(r, tx, ty), piece(r, tx, ty), ag_send, ag_recv.at[r, step], device(x=px, y=py)).start()

    def spread(r, direct):
        mine = piece(r, x, y)
        for s in range(NY):
            for h in range(2):
                for p in range(PAIRS):
                    mine[h, pl.ds((s * PAIRS + p) * 2, 2), :] = gathered[r, s, h, p]

        def send_all(p, carry):
            px, py = up(x, lax.rem(p, NX), NX), up(y, p // NX, NY)
            remote(mine, mine, ag_send, ag_recv.at[r, 2 + p // NX], device(x=px, y=py)).start()
            return carry

        def send_axes(d, carry):
            share(r, x, y, d, 0, 0)
            share(r, x, y, 0, d, 1)
            return carry

        if direct:
            lax.fori_loop(1, PLANE, send_all, 0)
        else:
            lax.fori_loop(1, NX, send_axes, 0)

    def pass_on(r):
        with scope("wrow"):
            waits(xbuf.at[r, :, :, pl.ds(0, (NX - 1) * LANES)], ag_recv.at[r, 0])

        def take(da, carry):
            tx, ty = shifted(da, 0)
            for db in range(1, NY):
                share(r, tx, ty, 0, db, 1)
            return carry

        lax.fori_loop(1, NX, take, 0)

    def halve(r):
        for da in (2, 1, 3, 0):
            a = up(my_a, da, NX)
            for db in (2, 1, 3):
                px, py = shifted(0, db)
                remote(
                    ybuf.at[r, up(my_b, db, NY), a], half.at[r, db - 1, a], half_send, half_recv.at[r, da],
                    device(x=px, y=py),
                ).start()

    def compute(r, direct, direct_sum, hold=False):
        if direct:
            up_gate = None
            for dy in (0, 1, 3, 2):
                with scope("wag"):
                    waits(xbuf.at[r, :, :, pl.ds(0, (NX if dy else NX - 1) * LANES)], ag_recv.at[r, 2 + dy])
                row = pl.ds(pl.multiple_of(up(y, NY - dy, NY) * NX * LANES, NX * LANES), NX * LANES)
                for h in range(2):
                    part = jnp.dot(xbuf[r, h, :, row], wup[h, row, :], preferred_element_type=jnp.float32)
                    up_gate = part if up_gate is None else up_gate + part
        else:
            with scope("wag"):
                waits(xbuf.at[r, :, :, pl.ds(0, (PLANE - NX) * LANES)], ag_recv.at[r, 1])
            up_gate = jnp.dot(xbuf[r, 0], wup[0], preferred_element_type=jnp.float32)
            up_gate = up_gate + jnp.dot(xbuf[r, 1], wup[1], preferred_element_type=jnp.float32)

        def swish(k):
            g, u = up_gate[:, k * 256 : k * 256 + 128], up_gate[:, k * 256 + 128 : k * 256 + 256]
            return (g / (1.0 + jnp.exp(-g)) * u).astype(jnp.bfloat16)

        act = jnp.concatenate([swish(0), swish(1)], axis=1)
        for dy in (2, 1, 3, 0):
            ty = up(y, dy, NY)
            cols = pl.ds(pl.multiple_of(ty * NX * LANES, NX * LANES), NX * LANES)
            for h in range(2):
                out = jnp.dot(act, wdown[h, :, cols], preferred_element_type=jnp.float32).astype(jnp.bfloat16)
                for tx in range(NX):
                    to_b, to_a = where_to(tx, ty)
                    ybuf[r, to_b, to_a, h] = out[:, tx * LANES : (tx + 1) * LANES]
            if not direct_sum:
                continue
            for dx in (2, 1, 3, 0):
                if dx == 0 and dy == 0:
                    continue
                tx = up(x, dx, NX)
                to_b, to_a = where_to(tx, ty)
                remote(
                    ybuf.at[r, to_b, to_a], whole.at[dy * NX + dx - 1], whole_send, whole_recv, device(x=tx, y=ty)
                ).start()
        if not direct_sum and not hold:
            halve(r)

    def quarter_sum(r):
        for da in (2, 1, 3, 0):
            a = up(my_a, da, NX)
            with scope("whalf"):
                waits(quarter.at[r], half_recv.at[r, da])
            acc = ybuf[r, my_b, a].astype(jnp.float32)
            for k in range(NY - 1):
                acc = acc + half[r, k, a].astype(jnp.float32)
            ybuf[r, my_b, a] = acc.astype(jnp.bfloat16)
            if da:
                px, py = shifted(da, 0)
                remote(
                    ybuf.at[r, my_b, a], quarter.at[r, da - 1], quarter_send, quarter_recv.at[r], device(x=px, y=py)
                ).start()

    def send_home(r, direct_sum):
        acc = ybuf[r, my_b, my_a].astype(jnp.float32)
        if direct_sum:
            with scope("wwhole"):
                waits(whole, whole_recv)
            for s in range(PLANE - 1):
                acc = acc + whole[s].astype(jnp.float32)
        else:
            with scope("wquart"):
                waits(quarter.at[r], quarter_recv.at[r])
            for s in range(NX - 1):
                acc = acc + quarter[r, s].astype(jnp.float32)
        total[...] = acc
        for s in range(NY):
            for h in range(2):
                for p in range(PAIRS):
                    homeward[r, s, h, p] = total[h, pl.ds((s * PAIRS + p) * 2, 2), :].astype(jnp.bfloat16)

        def send(k, carry):
            ty, h = k // 2, lax.rem(k, 2)
            tz = 2 * y + h
            dst = arrived.at[zh, zl]
            here = (r == zh) & (ty == y) & (tz == zl)

            @pl.when(here)
            def _():
                pltpu.make_async_copy(homeward.at[r, ty, h], dst, ret_recv).start()

            @pl.when(jnp.logical_not(here))
            def _():
                remote(homeward.at[r, ty, h], dst, ret_send, ret_recv, device(y=ty, zh=r, zl=tz)).start()
            return carry

        lax.fori_loop(0, 2 * NY, send, 0)

    with scope("wraw"):
        waits(wraw.at[:, pl.ds(0, 2 * UNITS)], load_sem.at[3])
        waits(wdown.at[:, pl.ds(0, UNITS)], load_sem.at[4])
    for h in range(2):
        wup[h, :, pl.ds(0, 256)] = wraw[h, pl.ds(0, 256), :].T

    @pl.when((c == 0) & (lax.rem(zh, 2) == 0))
    def _():
        lax.fori_loop(0, NY, to_region(jnp.where(high, ahead, behind)), 0)

    @pl.when((c == 0) & (lax.rem(zh, 2) == 0))
    def _():
        lax.fori_loop(0, NY, to_region(jnp.where(high, behind, ahead)), 0)

    @pl.when((c == 0) & (lax.rem(zh, 2) == 1))
    def _():
        lax.fori_loop(0, NY, to_region(0), 0)

    with scope("wS0"):
        waits(gathered.at[order[0]], disp_recv.at[order[0]])
    with scope("S0"):
        spread(order[0], True)
    @pl.when(c == 1)
    def _():
        lax.fori_loop(0, NY, to_region(jnp.where(lax.rem(zh, 2) == 0, ahead, 0)), 0)

        @pl.when(lax.rem(zh, 2) == 0)
        def _():
            lax.fori_loop(0, NY, to_region(behind), 0)

    with scope("R"):
        @pl.when(relays & (zh == 3))
        def _():
            second_leg(1, ahead, -6)

        @pl.when(relays)
        def _():
            second_leg(0, behind, 6)

        @pl.when(relays & (zh != 3))
        def _():
            second_leg(1, ahead, -6)
    for part, _, twin, _ in parts:
        remote(part, twin, twin_send, twin_recv, device(c=1 - c)).start()

    @pl.when(zh == 0)
    def _():
        with scope("wS1"):
            waits(gathered.at[order[1]], disp_recv.at[order[1]])
        with scope("S1"):
            spread(order[1], False)
        with scope("wtwin"):
            waits(wraw.at[:, pl.ds(0, 3 * UNITS)], twin_recv)
        for h in range(2):
            wup[h, :, pl.ds(256, 256)] = wraw[h, pl.ds(256, 256), :].T
        with scope("wS2"):
            waits(gathered.at[order[2]], disp_recv.at[order[2]])
        with scope("S2"):
            spread(order[2], False)
        with scope("A0"):
            compute(work[0], True, False)
        with scope("F1"):
            pass_on(order[1])
        with scope("wS3"):
            waits(gathered.at[order[3]], disp_recv.at[order[3]])
        with scope("S3"):
            spread(order[3], False)
        with scope("F2"):
            pass_on(order[2])
        with scope("A1"):
            compute(work[1], False, False)
        with scope("F3"):
            pass_on(order[3])
        with scope("A2"):
            compute(work[2], False, False)
        with scope("Q0"):
            quarter_sum(work[0])
        with scope("Q1"):
            quarter_sum(work[1])
        with scope("A3"):
            compute(work[3], False, True)
        with scope("Z0"):
            send_home(work[0], False)
        with scope("Q2"):
            quarter_sum(work[2])
        with scope("Z1"):
            send_home(work[1], False)
        with scope("Z2"):
            send_home(work[2], False)
        with scope("Z3"):
            send_home(work[3], True)

    @pl.when(zh == 2)
    def _():
        with scope("wtwin"):
            waits(wraw.at[:, pl.ds(0, 3 * UNITS)], twin_recv)
        for h in range(2):
            wup[h, :, pl.ds(256, 256)] = wraw[h, pl.ds(256, 256), :].T
        with scope("wS2"):
            waits(gathered.at[order[2]], disp_recv.at[order[2]])
        with scope("S2"):
            spread(order[2], True)
        with scope("wS1"):
            waits(gathered.at[order[1]], disp_recv.at[order[1]])
        with scope("S1"):
            spread(order[1], False)
        with scope("A0"):
            compute(work[0], True, True)
        @pl.when(c == 0)
        def _():
            with scope("wS3"):
                waits(gathered.at[order[3]], disp_recv.at[order[3]])
            with scope("S3"):
                spread(order[3], False)

        with scope("F1"):
            pass_on(order[1])
        with scope("A2"):
            compute(work[2], True, False, True)
        with scope("Z0"):
            send_home(work[0], True)
        @pl.when(c == 1)
        def _():
            with scope("wS3"):
                waits(gathered.at[order[3]], disp_recv.at[order[3]])
            with scope("S3"):
                spread(order[3], False)

        @pl.when(c == 0)
        def _():
            with scope("F3"):
                pass_on(order[3])

        with scope("A1"):
            compute(work[1], False, False)
        @pl.when(c == 1)
        def _():
            with scope("F3"):
                pass_on(order[3])

        @pl.when(c == 0)
        def _():
            with scope("A3"):
                compute(work[3], False, False, True)

        with scope("Q1"):
            quarter_sum(work[1])
        @pl.when(c == 0)
        def _():
            with scope("H3"):
                halve(work[3])

        @pl.when(c == 1)
        def _():
            with scope("A3"):
                compute(work[3], False, False)

        with scope("H2"):
            halve(work[2])
        with scope("Z1"):
            send_home(work[1], False)
        with scope("Q3"):
            quarter_sum(work[3])
        with scope("Q2"):
            quarter_sum(work[2])
        with scope("Z3"):
            send_home(work[3], False)
        with scope("Z2"):
            send_home(work[2], False)

    @pl.when(zh == 1)
    def _():
        with scope("wS1"):
            waits(gathered.at[order[1]], disp_recv.at[order[1]])
        with scope("S1"):
            spread(order[1], True)
        with scope("NL"):
            pl.semaphore_wait(ready, NY)
        lax.fori_loop(0, NY, to_region(2), 0)
        with scope("wtwin"):
            waits(wraw.at[:, pl.ds(0, 3 * UNITS)], twin_recv)
        for h in range(2):
            wup[h, :, pl.ds(256, 256)] = wraw[h, pl.ds(256, 256), :].T
        with scope("A0"):
            compute(work[0], True, False)
        with scope("wS2"):
            waits(gathered.at[order[2]], disp_recv.at[order[2]])
        with scope("S2"):
            spread(order[2], False)
        with scope("wS3"):
            waits(gathered.at[order[3]], disp_recv.at[order[3]])
        with scope("S3"):
            spread(order[3], False)
        with scope("F2"):
            pass_on(order[2])
        with scope("A1"):
            compute(work[1], True, True)
        with scope("F3"):
            pass_on(order[3])
        with scope("Q0"):
            quarter_sum(work[0])
        with scope("A2"):
            compute(work[2], False, False)
        with scope("Z1"):
            send_home(work[1], True)
        with scope("Z0"):
            send_home(work[0], False)
        with scope("A3"):
            compute(work[3], False, False)
        with scope("Q2"):
            quarter_sum(work[2])
        with scope("Z2"):
            send_home(work[2], False)
        with scope("Q3"):
            quarter_sum(work[3])
        with scope("Z3"):
            send_home(work[3], False)

    @pl.when(zh == 3)
    def _():
        with scope("wS1"):
            waits(gathered.at[order[1]], disp_recv.at[order[1]])
        with scope("S1"):
            spread(order[1], False)
        with scope("NL"):
            pl.semaphore_wait(ready, NY)
        lax.fori_loop(0, NY, to_region(2), 0)
        with scope("wtwin"):
            waits(wraw.at[:, pl.ds(0, 3 * UNITS)], twin_recv)
        for h in range(2):
            wup[h, :, pl.ds(256, 256)] = wraw[h, pl.ds(256, 256), :].T
        with scope("A0"):
            compute(work[0], True, False)
        with scope("F1"):
            pass_on(order[1])
        with scope("wS2"):
            waits(gathered.at[order[2]], disp_recv.at[order[2]])
        with scope("S2"):
            spread(order[2], False)
        with scope("wS3"):
            waits(gathered.at[order[3]], disp_recv.at[order[3]])
        with scope("S3"):
            spread(order[3], False)
        with scope("F2"):
            pass_on(order[2])
        with scope("A1"):
            compute(work[1], False, False)
        with scope("F3"):
            pass_on(order[3])
        with scope("Q0"):
            quarter_sum(work[0])
        with scope("A2"):
            compute(work[2], False, False)
        with scope("Q1"):
            quarter_sum(work[1])
        with scope("Z1"):
            send_home(work[1], False)
        with scope("A3"):
            compute(work[3], False, False)
        with scope("Q2"):
            quarter_sum(work[2])
        with scope("Z0"):
            send_home(work[0], False)
        with scope("Z2"):
            send_home(work[2], False)
        with scope("Q3"):
            quarter_sum(work[3])
        with scope("Z3"):
            send_home(work[3], False)

    with scope("wret"):
        waits(arrived, ret_recv)
    for e in range(EXPERTS):
        for p in range(PAIRS):
            part = arrived[0, e, p].astype(jnp.float32)
            for k in range(1, NZH):
                part = part + arrived[k, e, p].astype(jnp.float32)
            returned[pl.ds((e * PAIRS + p) * 2, 2), :] = part
    place = lax.broadcasted_iota(jnp.int32, (EXPERTS * SLOTS, tokens), 0)
    gates = gate_ref[...].astype(jnp.float32)
    combining = jnp.where(n_first == place, gates[0:1, :], 0.0) + jnp.where(n_second == place, gates[1:2, :], 0.0)
    mixed = lax.dot_general(
        combining, returned[...], (((0,), (0,)), ((), ())),
        preferred_element_type=jnp.float32, precision=lax.Precision.HIGHEST,
    )
    residual = hid[:, pl.ds(pl.multiple_of((zl * NX + x) * LANES, LANES), LANES)].astype(jnp.float32)
    out_ref[...] = (residual + mixed).astype(jnp.bfloat16)

    with scope("drain"):
        waits(wraw.at[:, pl.ds(0, 3 * UNITS)], twin_send)
        for _ in range(3):
            waits(gathered.at[1], disp_send)
        waits(gathered.at[0, pl.ds(0, 3)], disp_send)

        @pl.when(relays)
        def _():
            waits(gathered.at[pl.ds(0, 2)], disp_send)

        for r in range(NZH):
            waits(xbuf.at[r, :, :, pl.ds(0, (PLANE - 1) * LANES)], ag_send)
        for r in range(NZH - 1):
            waits(half.at[r], half_send)
            waits(quarter.at[r], quarter_send)

        whole_sum = (zh == 0) | (zh == 1) | (zh == 2)

        @pl.when(jnp.logical_not(whole_sum))
        def _():
            waits(half.at[0], half_send)
            waits(quarter.at[0], quarter_send)

        @pl.when(whole_sum)
        def _():
            waits(whole, whole_send)

        waits(arrived.at[pl.ds(0, 3)], ret_send)
        waits(arrived.at[3, pl.ds(0, 7)], ret_send)

        @pl.when((zl != 2 * y) & (zl != 2 * y + 1))
        def _():
            waits(arrived.at[3, 7], ret_send)


def local(hidden_in, expert_ids, gate_vals, w_gate, w_up, w_down):
    tokens, width = hidden_in.shape
    ids = jnp.swapaxes(expert_ids, 0, 1)
    gates = jnp.swapaxes(gate_vals, 0, 1)
    wg = jnp.swapaxes(w_gate[0], 0, 1)
    wu = jnp.swapaxes(w_up[0], 0, 1)
    bf16, f32 = jnp.bfloat16, jnp.float32
    dma, hbm, vmem = pltpu.SemaphoreType.DMA, pl.BlockSpec(memory_space=pltpu.HBM), pl.BlockSpec(memory_space=pltpu.VMEM)
    return pl.pallas_call(
        moe_kernel,
        name="moe",
        out_shape=jax.ShapeDtypeStruct((tokens, LANES), bf16),
        in_specs=[hbm] * 6,
        out_specs=vmem,
        scratch_shapes=[
            pltpu.VMEM((tokens, width), bf16),
            pltpu.VMEM((2, tokens), jnp.int32),
            pltpu.VMEM((2, tokens), bf16),
            pltpu.VMEM((2, 512, width // 2), bf16),
            pltpu.VMEM((2, width // 2, 512), bf16),
            pltpu.VMEM((2, 256, width // 2), bf16),
            pltpu.VMEM((2, NY, 2, PAIRS, 2, LANES), bf16),
            pltpu.VMEM((2, NY, 2, PAIRS, 2, LANES), bf16),
            pltpu.VMEM((NZH, NY, 2, PAIRS, 2, LANES), bf16),
            pltpu.VMEM((NZH, 2, ROWS, width // 2), bf16),
            pltpu.VMEM((NZH, NY, NX, 2, ROWS, LANES), bf16),
            pltpu.VMEM((NZH, NY - 1, NX, 2, ROWS, LANES), bf16),
            pltpu.VMEM((NZH, NX - 1, 2, ROWS, LANES), bf16),
            pltpu.VMEM((PLANE - 1, 2, ROWS, LANES), bf16),
            pltpu.VMEM((2, ROWS, LANES), f32),
            pltpu.VMEM((NZH, NY, 2, PAIRS, 2, LANES), bf16),
            pltpu.VMEM((NZH, NZL, PAIRS, 2, LANES), bf16),
            pltpu.VMEM((EXPERTS * SLOTS, LANES), f32),
            pltpu.SemaphoreType.REGULAR, dma((5,)), dma, dma, dma((2,)), dma, dma((4,)), dma, dma((4, 2 + NY)),
            dma, dma((4, NX)), dma, dma((4,)), dma, dma, dma, dma,
        ],
        compiler_params=pltpu.CompilerParams(
            collective_id=0, has_side_effects=True, vmem_limit_bytes=48 * 1024 * 1024
        ),
    )(*(pltpu.with_memory_space_constraint(a, pltpu.HBM) for a in (hidden_in, ids, gates, wg, wu, w_down[0])))


def solution(mesh):
    split = Mesh(mesh.devices.reshape(NY, NZH, NC, NZL, NX), AXES)
    return jax.shard_map(
        local,
        mesh=split,
        in_specs=(
            P(SEQ, None),
            P(SEQ, None),
            P(SEQ, None),
            P(ET, None, SEQ),
            P(ET, None, SEQ),
            P(ET, SEQ, None),
        ),
        out_specs=P(SEQ, ET),
        check_vma=False,
    )
```

```python
import jax
import jax.numpy as jnp
from jax import lax
from jax.experimental import pallas as pl
from jax.experimental.pallas import tpu as pltpu
from jax.sharding import Mesh
from jax.sharding import PartitionSpec as P

EXPERTS = 8
SLOTS = 10
PAIRS = SLOTS // 2
LANES = 128
AXES = ("y", "zh", "c", "zl", "x")
NY, NZH, NC, NZL, NX = 4, 4, 2, 8, 4
SEQ = ("y", "zh", "c")
ET = ("zl", "x")
ROWS = NY * SLOTS
UNITS = 112
PLANE = NX * NY
MESH = pl.DeviceIdType.MESH


def moe_kernel(
    hidden_any, ids_any, gate_any, wg_any, wu_any, wd_any,
    out_ref,
    hid, ids_ref, gate_ref, wraw, wup, wdown, picked, passed, gathered, xbuf, ybuf, half, quarter, whole, total, homeward, arrived, returned,
    ready, load_sem, twin_send, twin_recv, leg_recv, disp_send, disp_recv, ag_send, ag_recv,
    half_send, half_recv, quarter_send, quarter_recv, whole_send, whole_recv, ret_send, ret_recv,
):
    scope = jax.named_scope
    at = {name: lax.axis_index(name) for name in AXES}
    y, zh, c, zl, x = (at[name] for name in AXES)

    def device(**other):
        return {**at, **other}

    def remote(src, dst, send, recv, dev):
        return pltpu.make_async_remote_copy(
            src_ref=src, dst_ref=dst, send_sem=send, recv_sem=recv, device_id=dev, device_id_type=MESH
        )

    def waits(ref, sem):
        pltpu.make_async_copy(ref, ref, sem).wait()

    def up(v, d, n):
        return lax.rem(v + d, n)

    ahead, behind, across = up(zh, 1, NZH), up(zh, 3, NZH), up(zh, 2, NZH)

    barrier = pltpu.get_barrier_semaphore()

    def hello(**other):
        pl.semaphore_signal(barrier, inc=1, device_id=device(**other), device_id_type=MESH)

    def column(call, target):
        def body(d, carry):
            call(y=up(y, d, NY), zh=target)
            return carry

        lax.fori_loop(0, NY, body, 0)

    high, relays = zl >= NZL // 2, (zl >= 2) & (zl < 6)

    def along(step):
        z = lax.rem(zh * NZL + zl + step + NZH * NZL, NZH * NZL)
        return {"zh": z // NZL, "zl": lax.rem(z, NZL)}

    def hello_relay(d, carry):
        hello(y=up(y, d, NY), **along(jnp.where(high, 6, -6)))
        return carry

    def hello_line(d, carry):
        hello(zl=up(zl, d, NZL))
        return carry

    def hello_plane(p, carry):
        hello(x=up(x, lax.rem(p, NX), NX), y=up(y, p // NX, NY))
        return carry

    @pl.when(zh != 2)
    def _():
        column(hello, ahead)
        column(hello, behind)

    lax.fori_loop(0, NY, hello_relay, 0)

    @pl.when(relays)
    def _():
        hello(**along(6))
        hello(**along(-6))

    lax.fori_loop(1, NZL, hello_line, 0)
    lax.fori_loop(1, PLANE, hello_plane, 0)
    hello(c=1 - c)

    width = wdown.shape[2]
    small = [
        pltpu.make_async_copy(ids_any, ids_ref, load_sem.at[0]),
        pltpu.make_async_copy(gate_any, gate_ref, load_sem.at[1]),
        pltpu.make_async_copy(hidden_any, hid, load_sem.at[2]),
    ]
    parts = []
    for h in range(2):
        for ty in range(NY):
            cols, to = pl.ds((2 * ty + h) * NX * LANES, NX * LANES), pl.ds(ty * NX * LANES, NX * LANES)
            for k, (weight, buf, own, twin) in enumerate(
                ((wg_any, wraw, 0, 256), (wu_any, wraw, 128, 384), (wd_any, wdown, 0, 128))
            ):
                parts.append((
                    weight.at[:, cols], buf.at[h, pl.ds(own, UNITS), to], buf.at[h, pl.ds(twin, UNITS), to], 3 + k // 2
                ))
    loads = [pltpu.make_async_copy(part, own, load_sem.at[sem]) for part, own, _, sem in parts]
    for load in small + loads:
        load.start()
    blank = jnp.zeros((128 - UNITS, width), jnp.bfloat16)
    for h in range(2):
        for k in range(4):
            wraw[h, pl.ds(k * 128 + UNITS, 128 - UNITS), :] = blank
        for k in range(2):
            wdown[h, pl.ds(k * 128 + UNITS, 128 - UNITS), :] = blank
    small[0].wait()
    small[1].wait()

    tokens = ids_ref.shape[1]
    ids = ids_ref[...]
    expert = lax.broadcasted_iota(jnp.int32, (EXPERTS, tokens), 0)
    first, second = ids[0:1, :], ids[1:2, :]
    named = (jnp.where(first == expert, 1.0, 0.0) + jnp.where(second == expert, 1.0, 0.0)).astype(jnp.float32)
    before = jnp.where(
        lax.broadcasted_iota(jnp.int32, (tokens, tokens), 0) < lax.broadcasted_iota(jnp.int32, (tokens, tokens), 1),
        1.0, 0.0,
    ).astype(jnp.float32)
    earlier = jnp.dot(named, before, preferred_element_type=jnp.float32)

    def number(chosen):
        slot = jnp.sum(jnp.where(chosen == expert, earlier, 0.0), axis=0, keepdims=True)
        return chosen * SLOTS + slot.astype(jnp.int32)

    n_first, n_second = number(first), number(second)
    slot = lax.broadcasted_iota(jnp.int32, (16, tokens), 0)

    def placing(expert_here):
        wanted = jnp.where(slot < SLOTS, slot + expert_here * SLOTS, -1)
        return (
            jnp.where(n_first == wanted, 1.0, 0.0) + jnp.where(n_second == wanted, 1.0, 0.0)
        ).astype(jnp.bfloat16)

    places = jnp.concatenate([placing(zl), placing(lax.rem(zl + NZL // 2, NZL))], axis=0)
    small[2].wait()
    for j in range(NZL):
        block = hid[:, pl.ds(pl.multiple_of((j * NX + x) * LANES, LANES), LANES)]
        rows = jnp.dot(places, block, preferred_element_type=jnp.float32)
        for k in range(2):
            for p in range(PAIRS):
                picked[k, j // 2, j % 2, p] = rows[16 * k + 2 * p : 16 * k + 2 * p + 2].astype(jnp.bfloat16)

    with scope("w_barrier"):
        pl.semaphore_wait(barrier, jnp.where(lax.rem(zh, 2) == 0, 2 * NY, NY) + (NZL - 1) + (PLANE - 1) + 2 + jnp.where(relays, 2 * NY, 0))

    order = (
        jnp.where(zh == 0, 0, jnp.where(zh == 1, 1, jnp.where(zh == 2, 2, 3))),
        jnp.where(zh == 0, 1, jnp.where(zh == 1, 0, jnp.where(zh == 2, 1, 0))),
        jnp.where(zh == 0, 3, jnp.where(zh == 1, 2, jnp.where(zh == 2, 0, 1))),
        jnp.where(zh == 0, 2, jnp.where(zh == 1, 3, jnp.where(zh == 2, 3, 2))),
    )
    work = (
        jnp.where(zh == 0, 0, jnp.where(zh == 1, 1, jnp.where(zh == 2, 0, 3))),
        jnp.where(zh == 0, 1, jnp.where(zh == 1, 0, jnp.where(zh == 2, 1, 0))),
        jnp.where(zh == 0, 3, jnp.where(zh == 1, 2, jnp.where(zh == 2, 2, 1))),
        jnp.where(zh == 0, 2, jnp.where(zh == 1, 3, jnp.where(zh == 2, 3, 2))),
    )

    def say_ready(**other):
        pl.semaphore_signal(ready, inc=1, device_id=device(**other), device_id_type=MESH)

    @pl.when(high)
    def _():
        remote(picked.at[1], passed.at[0], disp_send, leg_recv.at[0], device(**along(6))).start()

    @pl.when(jnp.logical_not(high))
    def _():
        remote(picked.at[1], passed.at[1], disp_send, leg_recv.at[1], device(**along(-6))).start()

    def to_region(target):
        def send(d, carry):
            ty = up(y, d, NY)
            remote(
                picked.at[0, ty], gathered.at[zh, y], disp_send, disp_recv.at[zh], device(y=ty, zh=target)
            ).start()
            return carry
        return send

    lax.fori_loop(1, NY, to_region(zh), 0)
    pltpu.make_async_copy(picked.at[0, y], gathered.at[zh, y], disp_recv.at[zh]).start()

    def second_leg(way, source, step):
        with scope("leg"):
            waits(passed.at[way], leg_recv.at[way])

        def send(d, carry):
            ty = up(y, d, NY)
            remote(
                passed.at[way, ty], gathered.at[source, y], disp_send, disp_recv.at[source], device(y=ty, **along(step))
            ).start()
            return carry

        lax.fori_loop(0, NY, send, 0)

    def shifted(da, db):
        return up(x, da * (1 - c) + db * c, NX), up(y, da * c + db * (1 - c), NY)

    def where_to(tx, ty):
        return ty * (1 - c) + tx * c, tx * (1 - c) + ty * c

    my_b, my_a = where_to(x, y)

    def piece(r, tx, ty):
        return xbuf.at[r, :, :, pl.ds(pl.multiple_of((ty * NX + tx) * LANES, LANES), LANES)]

    def share(r, tx, ty, da, db, step):
        px, py = shifted(da, db)
        remote(piece(r, tx, ty), piece(r, tx, ty), ag_send, ag_recv.at[r, step], device(x=px, y=py)).start()

    def spread(r, direct):
        mine = piece(r, x, y)
        for s in range(NY):
            for h in range(2):
                for p in range(PAIRS):
                    mine[h, pl.ds((s * PAIRS + p) * 2, 2), :] = gathered[r, s, h, p]

        def send_all(p, carry):
            px, py = up(x, lax.rem(p, NX), NX), up(y, p // NX, NY)
            remote(mine, mine, ag_send, ag_recv.at[r, 2 + p // NX], device(x=px, y=py)).start()
            return carry

        def send_axes(d, carry):
            share(r, x, y, d, 0, 0)
            share(r, x, y, 0, d, 1)
            return carry

        if direct:
            lax.fori_loop(1, PLANE, send_all, 0)
        else:
            lax.fori_loop(1, NX, send_axes, 0)

    def pass_on(r):
        with scope("wrow"):
            waits(xbuf.at[r, :, :, pl.ds(0, (NX - 1) * LANES)], ag_recv.at[r, 0])

        def take(da, carry):
            tx, ty = shifted(da, 0)
            for db in range(1, NY):
                share(r, tx, ty, 0, db, 1)
            return carry

        lax.fori_loop(1, NX, take, 0)

    def halve(r):
        for da in (2, 1, 3, 0):
            a = up(my_a, da, NX)
            for db in (2, 1, 3):
                px, py = shifted(0, db)
                remote(
                    ybuf.at[r, up(my_b, db, NY), a], half.at[r, db - 1, a], half_send, half_recv.at[r, da],
                    device(x=px, y=py),
                ).start()

    def compute(r, direct, direct_sum, hold=False):
        if direct:
            up_gate = None
            for dy in (0, 1, 3, 2):
                with scope("wag"):
                    waits(xbuf.at[r, :, :, pl.ds(0, (NX if dy else NX - 1) * LANES)], ag_recv.at[r, 2 + dy])
                row = pl.ds(pl.multiple_of(up(y, NY - dy, NY) * NX * LANES, NX * LANES), NX * LANES)
                for h in range(2):
                    part = jnp.dot(xbuf[r, h, :, row], wup[h, row, :], preferred_element_type=jnp.float32)
                    up_gate = part if up_gate is None else up_gate + part
        else:
            with scope("wag"):
                waits(xbuf.at[r, :, :, pl.ds(0, (PLANE - NX) * LANES)], ag_recv.at[r, 1])
            up_gate = jnp.dot(xbuf[r, 0], wup[0], preferred_element_type=jnp.float32)
            up_gate = up_gate + jnp.dot(xbuf[r, 1], wup[1], preferred_element_type=jnp.float32)

        def swish(k):
            g, u = up_gate[:, k * 256 : k * 256 + 128], up_gate[:, k * 256 + 128 : k * 256 + 256]
            return (g / (1.0 + jnp.exp(-g)) * u).astype(jnp.bfloat16)

        act = jnp.concatenate([swish(0), swish(1)], axis=1)
        for dy in (2, 1, 3, 0):
            ty = up(y, dy, NY)
            cols = pl.ds(pl.multiple_of(ty * NX * LANES, NX * LANES), NX * LANES)
            for h in range(2):
                out = jnp.dot(act, wdown[h, :, cols], preferred_element_type=jnp.float32).astype(jnp.bfloat16)
                for tx in range(NX):
                    to_b, to_a = where_to(tx, ty)
                    ybuf[r, to_b, to_a, h] = out[:, tx * LANES : (tx + 1) * LANES]
            if not direct_sum:
                continue
            for dx in (2, 1, 3, 0):
                if dx == 0 and dy == 0:
                    continue
                tx = up(x, dx, NX)
                to_b, to_a = where_to(tx, ty)
                remote(
                    ybuf.at[r, to_b, to_a], whole.at[dy * NX + dx - 1], whole_send, whole_recv, device(x=tx, y=ty)
                ).start()
        if not direct_sum and not hold:
            halve(r)

    def quarter_sum(r):
        for da in (2, 1, 3, 0):
            a = up(my_a, da, NX)
            with scope("whalf"):
                waits(quarter.at[r], half_recv.at[r, da])
            acc = ybuf[r, my_b, a].astype(jnp.float32)
            for k in range(NY - 1):
                acc = acc + half[r, k, a].astype(jnp.float32)
            ybuf[r, my_b, a] = acc.astype(jnp.bfloat16)
            if da:
                px, py = shifted(da, 0)
                remote(
                    ybuf.at[r, my_b, a], quarter.at[r, da - 1], quarter_send, quarter_recv.at[r], device(x=px, y=py)
                ).start()

    def send_home(r, direct_sum):
        acc = ybuf[r, my_b, my_a].astype(jnp.float32)
        if direct_sum:
            with scope("wwhole"):
                waits(whole, whole_recv)
            for s in range(PLANE - 1):
                acc = acc + whole[s].astype(jnp.float32)
        else:
            with scope("wquart"):
                waits(quarter.at[r], quarter_recv.at[r])
            for s in range(NX - 1):
                acc = acc + quarter[r, s].astype(jnp.float32)
        total[...] = acc
        for s in range(NY):
            for h in range(2):
                for p in range(PAIRS):
                    homeward[r, s, h, p] = total[h, pl.ds((s * PAIRS + p) * 2, 2), :].astype(jnp.bfloat16)

        def send(k, carry):
            ty, h = k // 2, lax.rem(k, 2)
            tz = 2 * y + h
            dst = arrived.at[zh, zl]
            here = (r == zh) & (ty == y) & (tz == zl)

            @pl.when(here)
            def _():
                pltpu.make_async_copy(homeward.at[r, ty, h], dst, ret_recv).start()

            @pl.when(jnp.logical_not(here))
            def _():
                remote(homeward.at[r, ty, h], dst, ret_send, ret_recv, device(y=ty, zh=r, zl=tz)).start()
            return carry

        lax.fori_loop(0, 2 * NY, send, 0)

    with scope("wraw"):
        waits(wraw.at[:, pl.ds(0, 2 * UNITS)], load_sem.at[3])
        waits(wdown.at[:, pl.ds(0, UNITS)], load_sem.at[4])
    for h in range(2):
        wup[h, :, pl.ds(0, 256)] = wraw[h, pl.ds(0, 256), :].T

    @pl.when((c == 0) & (lax.rem(zh, 2) == 0))
    def _():
        lax.fori_loop(0, NY, to_region(jnp.where(high, ahead, behind)), 0)

    @pl.when((c == 0) & (lax.rem(zh, 2) == 0))
    def _():
        lax.fori_loop(0, NY, to_region(jnp.where(high, behind, ahead)), 0)

    @pl.when((c == 0) & (lax.rem(zh, 2) == 1))
    def _():
        lax.fori_loop(0, NY, to_region(0), 0)

    with scope("wS0"):
        waits(gathered.at[order[0]], disp_recv.at[order[0]])
    @pl.when(zh == 2)
    def _():
        column(say_ready, ahead)
        column(say_ready, behind)

    with scope("S0"):
        spread(order[0], True)
    @pl.when(c == 1)
    def _():
        lax.fori_loop(0, NY, to_region(jnp.where(lax.rem(zh, 2) == 0, ahead, 0)), 0)

        @pl.when(lax.rem(zh, 2) == 0)
        def _():
            lax.fori_loop(0, NY, to_region(behind), 0)

    with scope("R"):
        @pl.when(relays & (zh == 3))
        def _():
            second_leg(1, ahead, -6)

        @pl.when(relays)
        def _():
            second_leg(0, behind, 6)

        @pl.when(relays & (zh != 3))
        def _():
            second_leg(1, ahead, -6)
    for part, _, twin, _ in parts:
        remote(part, twin, twin_send, twin_recv, device(c=1 - c)).start()

    @pl.when(zh == 0)
    def _():
        with scope("wS1"):
            waits(gathered.at[order[1]], disp_recv.at[order[1]])
        with scope("S1"):
            spread(order[1], False)
        with scope("wtwin"):
            waits(wraw.at[:, pl.ds(0, 3 * UNITS)], twin_recv)
        for h in range(2):
            wup[h, :, pl.ds(256, 256)] = wraw[h, pl.ds(256, 256), :].T
        with scope("wS2"):
            waits(gathered.at[order[2]], disp_recv.at[order[2]])
        with scope("S2"):
            spread(order[2], False)
        with scope("A0"):
            compute(work[0], True, False)
        with scope("F1"):
            pass_on(order[1])
        with scope("wS3"):
            waits(gathered.at[order[3]], disp_recv.at[order[3]])
        with scope("S3"):
            spread(order[3], False)
        with scope("F2"):
            pass_on(order[2])
        with scope("A1"):
            compute(work[1], False, False)
        with scope("F3"):
            pass_on(order[3])
        with scope("A2"):
            compute(work[2], False, False)
        with scope("Q0"):
            quarter_sum(work[0])
        with scope("Q1"):
            quarter_sum(work[1])
        with scope("A3"):
            compute(work[3], False, True)
        with scope("Z0"):
            send_home(work[0], False)
        with scope("Q2"):
            quarter_sum(work[2])
        with scope("Z1"):
            send_home(work[1], False)
        with scope("Z2"):
            send_home(work[2], False)
        with scope("Z3"):
            send_home(work[3], True)

    @pl.when(zh == 2)
    def _():
        with scope("wtwin"):
            waits(wraw.at[:, pl.ds(0, 3 * UNITS)], twin_recv)
        for h in range(2):
            wup[h, :, pl.ds(256, 256)] = wraw[h, pl.ds(256, 256), :].T
        with scope("wS2"):
            waits(gathered.at[order[2]], disp_recv.at[order[2]])
        with scope("S2"):
            spread(order[2], True)
        with scope("wS1"):
            waits(gathered.at[order[1]], disp_recv.at[order[1]])
        with scope("S1"):
            spread(order[1], False)
        with scope("A0"):
            compute(work[0], True, True)
        @pl.when(c == 0)
        def _():
            with scope("wS3"):
                waits(gathered.at[order[3]], disp_recv.at[order[3]])
            with scope("S3"):
                spread(order[3], False)

        with scope("F1"):
            pass_on(order[1])
        with scope("A2"):
            compute(work[2], True, False, True)
        with scope("Z0"):
            send_home(work[0], True)
        @pl.when(c == 1)
        def _():
            with scope("wS3"):
                waits(gathered.at[order[3]], disp_recv.at[order[3]])
            with scope("S3"):
                spread(order[3], False)

        @pl.when(c == 0)
        def _():
            with scope("F3"):
                pass_on(order[3])

        with scope("A1"):
            compute(work[1], False, False)
        @pl.when(c == 1)
        def _():
            with scope("F3"):
                pass_on(order[3])

        @pl.when(c == 0)
        def _():
            with scope("A3"):
                compute(work[3], False, False, True)

        with scope("Q1"):
            quarter_sum(work[1])
        @pl.when(c == 0)
        def _():
            with scope("H3"):
                halve(work[3])

        @pl.when(c == 1)
        def _():
            with scope("A3"):
                compute(work[3], False, False)

        with scope("H2"):
            halve(work[2])
        with scope("Z1"):
            send_home(work[1], False)
        with scope("Q3"):
            quarter_sum(work[3])
        with scope("Q2"):
            quarter_sum(work[2])
        with scope("Z3"):
            send_home(work[3], False)
        with scope("Z2"):
            send_home(work[2], False)

    @pl.when(zh == 1)
    def _():
        with scope("NL"):
            pl.semaphore_wait(ready, NY)
        lax.fori_loop(0, NY, to_region(2), 0)
        with scope("wS1"):
            waits(gathered.at[order[1]], disp_recv.at[order[1]])
        with scope("S1"):
            spread(order[1], True)
        with scope("wtwin"):
            waits(wraw.at[:, pl.ds(0, 3 * UNITS)], twin_recv)
        for h in range(2):
            wup[h, :, pl.ds(256, 256)] = wraw[h, pl.ds(256, 256), :].T
        with scope("A0"):
            compute(work[0], True, False)
        with scope("wS2"):
            waits(gathered.at[order[2]], disp_recv.at[order[2]])
        with scope("S2"):
            spread(order[2], False)
        with scope("wS3"):
            waits(gathered.at[order[3]], disp_recv.at[order[3]])
        with scope("S3"):
            spread(order[3], False)
        with scope("F2"):
            pass_on(order[2])
        with scope("A1"):
            compute(work[1], True, True)
        with scope("F3"):
            pass_on(order[3])
        with scope("Q0"):
            quarter_sum(work[0])
        with scope("A2"):
            compute(work[2], False, False)
        with scope("Z1"):
            send_home(work[1], True)
        with scope("Z0"):
            send_home(work[0], False)
        with scope("A3"):
            compute(work[3], False, False)
        with scope("Q2"):
            quarter_sum(work[2])
        with scope("Z2"):
            send_home(work[2], False)
        with scope("Q3"):
            quarter_sum(work[3])
        with scope("Z3"):
            send_home(work[3], False)

    @pl.when(zh == 3)
    def _():
        with scope("NL"):
            pl.semaphore_wait(ready, NY)
        lax.fori_loop(0, NY, to_region(2), 0)
        with scope("wS1"):
            waits(gathered.at[order[1]], disp_recv.at[order[1]])
        with scope("S1"):
            spread(order[1], False)
        with scope("wtwin"):
            waits(wraw.at[:, pl.ds(0, 3 * UNITS)], twin_recv)
        for h in range(2):
            wup[h, :, pl.ds(256, 256)] = wraw[h, pl.ds(256, 256), :].T
        with scope("A0"):
            compute(work[0], True, False)
        with scope("F1"):
            pass_on(order[1])
        with scope("wS2"):
            waits(gathered.at[order[2]], disp_recv.at[order[2]])
        with scope("S2"):
            spread(order[2], False)
        with scope("wS3"):
            waits(gathered.at[order[3]], disp_recv.at[order[3]])
        with scope("S3"):
            spread(order[3], False)
        with scope("F2"):
            pass_on(order[2])
        with scope("A1"):
            compute(work[1], False, False)
        with scope("F3"):
            pass_on(order[3])
        with scope("Q0"):
            quarter_sum(work[0])
        with scope("A2"):
            compute(work[2], False, False)
        with scope("Q1"):
            quarter_sum(work[1])
        with scope("Z1"):
            send_home(work[1], False)
        with scope("A3"):
            compute(work[3], False, False)
        with scope("Q2"):
            quarter_sum(work[2])
        with scope("Z0"):
            send_home(work[0], False)
        with scope("Z2"):
            send_home(work[2], False)
        with scope("Q3"):
            quarter_sum(work[3])
        with scope("Z3"):
            send_home(work[3], False)

    with scope("wret"):
        waits(arrived, ret_recv)
    for e in range(EXPERTS):
        for p in range(PAIRS):
            part = arrived[0, e, p].astype(jnp.float32)
            for k in range(1, NZH):
                part = part + arrived[k, e, p].astype(jnp.float32)
            returned[pl.ds((e * PAIRS + p) * 2, 2), :] = part
    place = lax.broadcasted_iota(jnp.int32, (EXPERTS * SLOTS, tokens), 0)
    gates = gate_ref[...].astype(jnp.float32)
    combining = jnp.where(n_first == place, gates[0:1, :], 0.0) + jnp.where(n_second == place, gates[1:2, :], 0.0)
    mixed = lax.dot_general(
        combining, returned[...], (((0,), (0,)), ((), ())),
        preferred_element_type=jnp.float32, precision=lax.Precision.HIGHEST,
    )
    residual = hid[:, pl.ds(pl.multiple_of((zl * NX + x) * LANES, LANES), LANES)].astype(jnp.float32)
    out_ref[...] = (residual + mixed).astype(jnp.bfloat16)

    with scope("drain"):
        waits(wraw.at[:, pl.ds(0, 3 * UNITS)], twin_send)
        for _ in range(3):
            waits(gathered.at[1], disp_send)
        waits(gathered.at[0, pl.ds(0, 3)], disp_send)

        @pl.when(relays)
        def _():
            waits(gathered.at[pl.ds(0, 2)], disp_send)

        for r in range(NZH):
            waits(xbuf.at[r, :, :, pl.ds(0, (PLANE - 1) * LANES)], ag_send)
        for r in range(NZH - 1):
            waits(half.at[r], half_send)
            waits(quarter.at[r], quarter_send)

        whole_sum = (zh == 0) | (zh == 1) | (zh == 2)

        @pl.when(jnp.logical_not(whole_sum))
        def _():
            waits(half.at[0], half_send)
            waits(quarter.at[0], quarter_send)

        @pl.when(whole_sum)
        def _():
            waits(whole, whole_send)

        waits(arrived.at[pl.ds(0, 3)], ret_send)
        waits(arrived.at[3, pl.ds(0, 7)], ret_send)

        @pl.when((zl != 2 * y) & (zl != 2 * y + 1))
        def _():
            waits(arrived.at[3, 7], ret_send)


def local(hidden_in, expert_ids, gate_vals, w_gate, w_up, w_down):
    tokens, width = hidden_in.shape
    ids = jnp.swapaxes(expert_ids, 0, 1)
    gates = jnp.swapaxes(gate_vals, 0, 1)
    wg = jnp.swapaxes(w_gate[0], 0, 1)
    wu = jnp.swapaxes(w_up[0], 0, 1)
    bf16, f32 = jnp.bfloat16, jnp.float32
    dma, hbm, vmem = pltpu.SemaphoreType.DMA, pl.BlockSpec(memory_space=pltpu.HBM), pl.BlockSpec(memory_space=pltpu.VMEM)
    return pl.pallas_call(
        moe_kernel,
        name="moe",
        out_shape=jax.ShapeDtypeStruct((tokens, LANES), bf16),
        in_specs=[hbm] * 6,
        out_specs=vmem,
        scratch_shapes=[
            pltpu.VMEM((tokens, width), bf16),
            pltpu.VMEM((2, tokens), jnp.int32),
            pltpu.VMEM((2, tokens), bf16),
            pltpu.VMEM((2, 512, width // 2), bf16),
            pltpu.VMEM((2, width // 2, 512), bf16),
            pltpu.VMEM((2, 256, width // 2), bf16),
            pltpu.VMEM((2, NY, 2, PAIRS, 2, LANES), bf16),
            pltpu.VMEM((2, NY, 2, PAIRS, 2, LANES), bf16),
            pltpu.VMEM((NZH, NY, 2, PAIRS, 2, LANES), bf16),
            pltpu.VMEM((NZH, 2, ROWS, width // 2), bf16),
            pltpu.VMEM((NZH, NY, NX, 2, ROWS, LANES), bf16),
            pltpu.VMEM((NZH, NY - 1, NX, 2, ROWS, LANES), bf16),
            pltpu.VMEM((NZH, NX - 1, 2, ROWS, LANES), bf16),
            pltpu.VMEM((PLANE - 1, 2, ROWS, LANES), bf16),
            pltpu.VMEM((2, ROWS, LANES), f32),
            pltpu.VMEM((NZH, NY, 2, PAIRS, 2, LANES), bf16),
            pltpu.VMEM((NZH, NZL, PAIRS, 2, LANES), bf16),
            pltpu.VMEM((EXPERTS * SLOTS, LANES), f32),
            pltpu.SemaphoreType.REGULAR, dma((5,)), dma, dma, dma((2,)), dma, dma((4,)), dma, dma((4, 2 + NY)),
            dma, dma((4, NX)), dma, dma((4,)), dma, dma, dma, dma,
        ],
        compiler_params=pltpu.CompilerParams(
            collective_id=0, has_side_effects=True, vmem_limit_bytes=48 * 1024 * 1024
        ),
    )(*(pltpu.with_memory_space_constraint(a, pltpu.HBM) for a in (hidden_in, ids, gates, wg, wu, w_down[0])))


def solution(mesh):
    split = Mesh(mesh.devices.reshape(NY, NZH, NC, NZL, NX), AXES)
    return jax.shard_map(
        local,
        mesh=split,
        in_specs=(
            P(SEQ, None),
            P(SEQ, None),
            P(SEQ, None),
            P(ET, None, SEQ),
            P(ET, None, SEQ),
            P(ET, SEQ, None),
        ),
        out_specs=P(SEQ, ET),
        check_vma=False,
    )
```
